256 devices in a mesh: obs: 64 (over z, y, core), rep: 4 (over x).
Axes of the slice: x: 4, y: 4, z: 8, core: 2. Of those that a mesh axis runs over, the one named last changes fastest.
Arguments:
- jacobians: float32 [18, 8388608], P(None, ('obs', 'rep')), may hold values from -3 to 3
- residuals: float32 [2, 8388608], P(None, ('obs', 'rep')), may hold values from -6 to 6
- camera_local: int32 [8388608], P(('obs', 'rep')), may hold values from 0 to 1023
- bucket_counts: int32 [256, 64], P(('obs', 'rep')), may hold values from 1 to 512, as said below
- camera_map: int32 [65536], replicated, may hold values from 0 to 65535, each once
Outputs:
- gradient: float32 [9, 65536], replicated
- camera_blocks: float32 [81, 65536], P(None, 'obs')
The draws below stay inside these ranges and needn't reach their ends.
Inputs may be any that keep to these rules, and one draw needn't show every extreme that they name: bucket_counts[s, d] counts the leading live slots of bucket d of source block s; exactly one destination d has all 512 slots live from every source block, and every other bucket has at most 256 live slots. A slot in bucket d names camera slot d * 1024 + camera_local. `camera_map`: each camera id appears once.
All inputs are finite; a program needn't handle non-finite values.
Results may differ from the reference program's by a relative error of at most 0.0003.
Values sent between devices are 32-bit elements; how exact they have to be, the bound alone decides.
No kernel may reach another device: no remote copies, remote signals or barrier semaphores. Data moves between devices by JAX's collectives and lax.ppermute only.
A program may use at most 192 MiB of HBM per device.

```python
import math
import jax
import jax.numpy as jnp
import numpy as np
from jax import lax

CAM_DEV = 1024
CAP = 512
CAM = 65536
SLOTS = 8388608
N_OBS = 64
N_REP = 4


def draw_bucket_counts(key, part):
    key_hot = jax.random.fold_in(key, 11)
    key_full = jax.random.fold_in(key, 12)
    key_base = jax.random.fold_in(key, 13)
    hotness = jax.random.randint(key_hot, (N_OBS,), 1, 4)
    full_column = jax.random.randint(key_full, (), 0, N_OBS)
    baseline = jax.random.randint(key_base, (N_OBS * N_REP, N_OBS), CAP // 4, CAP // 2 + 1)
    counts = jnp.minimum(CAP // 2, baseline * hotness[None, :] // 2)
    counts = jnp.maximum(counts, 1)
    column_ids = jnp.arange(N_OBS, dtype=jnp.int32)
    counts = jnp.where(column_ids[None, :] == full_column, CAP, counts)
    return counts.astype(jnp.int32)


def set_ends(drawn, rng, low, largest):
    index_at = [jax.random.randint(jax.random.fold_in(rng, axis), (), 0, length) for axis, length in enumerate(drawn.shape)]
    widest = drawn.shape.index(max(drawn.shape))
    neighbour = index_at[:widest] + [(index_at[widest] + 1) % drawn.shape[widest]] + index_at[widest + 1:]
    return drawn.at[tuple(index_at)].set(low).at[tuple(neighbour)].set(largest)


def block_scale(rng, dims, pieces, smallest, high):
    level, own = 1.0, jax.random.fold_in(rng, 6)
    for dim, shards_of in pieces:
        heights = jnp.exp(jax.random.uniform(jax.random.fold_in(own, dim), (shards_of,), jnp.float32, smallest / len(pieces), high / len(pieces)))
        level = level * jnp.repeat(heights, dims[dim] // shards_of).reshape([-1 if axis == dim else 1 for axis in range(len(dims))])
    return level


def rank_bounds(amount, skew):
    loads = [(1 << 20) // math.isqrt(grade ** skew) + 1 for grade in range(1, amount + 1)]
    scale = 1 + sum(loads) // (1 << 30)
    return np.cumsum(np.array([max(1, weight // scale) for weight in loads]))


def ranked_ids(key, dims, count, lean):
    grid = rank_bounds(count, lean)
    ticket = jax.random.randint(jax.random.fold_in(key, 1), dims, 0, int(grid[count - 1]))
    grade = jnp.searchsorted(jnp.asarray(grid, jnp.int32), ticket, side="right")
    return jax.random.permutation(jax.random.fold_in(key, 2), count)[grade].astype(jnp.int32)


def normal_values(rng, shape, width, most, shards=(), kind=jnp.bfloat16):
    level = block_scale(rng, shape, shards, -0.22, 0.18) if shards else 1.0
    values = jax.random.normal(rng, shape, jnp.float32) * width * level
    return jnp.minimum(jnp.maximum(values, -most), most).astype(kind)


def setup_inputs(seed: int = 0) -> dict:
    key_of = jax.random.split(jax.random.key(seed), 6)
    return {
        "jacobians": normal_values(key_of[0], (18, SLOTS), 0.5, 3.0, ((1, 256),), jnp.float32),
        "residuals": normal_values(key_of[1], (2, SLOTS), 1.0, 6.0, ((1, 256),), jnp.float32),
        "camera_local": set_ends(ranked_ids(key_of[2], (SLOTS,), CAM_DEV, 1), jax.random.fold_in(key_of[2], 3), 0, CAM_DEV - 1).astype(jnp.int32),
        "bucket_counts": draw_bucket_counts(jax.random.fold_in(key_of[5], 71), 0),
        "camera_map": jax.random.permutation(key_of[4], CAM).astype(jnp.int32),
    }


def observation_terms(jacobs, resids):
    leading_row = jacobs[0:9]
    trailing_row = jacobs[9:18]
    gradient_terms = leading_row * resids[0:1] + trailing_row * resids[1:2]
    block_terms = leading_row[:, None] * leading_row[None, :] + trailing_row[:, None] * trailing_row[None, :]
    block_terms = block_terms.reshape((81,) + leading_row.shape[1:])
    return jnp.concatenate([gradient_terms, block_terms], axis=0)


def reference(jacobians, residuals, camera_local, bucket_counts, camera_map):
    sources = N_OBS * N_REP
    columns = N_OBS * CAP
    jac_blocks = jnp.moveaxis(jacobians.reshape(18, sources, columns), 1, 0)
    res_blocks = jnp.moveaxis(residuals.reshape(2, sources, columns), 1, 0)
    cam_blocks = camera_local.reshape(sources, columns)
    position = jnp.arange(columns, dtype=jnp.int32)
    target = position // CAP
    within = position % CAP

    def accumulate(summed, inputs):
        jac_here, res_here, cam_here, count_here = inputs
        live_mask = (within < count_here[target]).astype(jnp.float32)
        obs_terms = observation_terms(jac_here * live_mask, res_here * live_mask)
        segment = (target * CAM_DEV + cam_here).astype(jnp.int32)
        return summed + jax.ops.segment_sum(obs_terms.T, segment, num_segments=CAM), None

    summed, unused = lax.scan(accumulate, jnp.zeros((CAM, 90), jnp.float32), (jac_blocks, res_blocks, cam_blocks, bucket_counts))
    slot_gradient = summed[:, :9].T
    camera_blocks = summed[:, 9:].T
    gradient = jnp.zeros((9, CAM), jnp.float32).at[:, camera_map].set(slot_gradient)
    return gradient, camera_blocks
```

```python
import jax
import jax.numpy as jnp
from jax import lax
from jax.experimental import pallas as pl
from jax.experimental.pallas import tpu as pltpu
from jax.sharding import Mesh
from jax.sharding import PartitionSpec as P

CAM_DEV = 1024
HALF = 256
LANES = 128
SPAN = 256
QUARTERS = CAM_DEV // SPAN
CAMS = 9
PAIRS = 45
TERMS = 56
VALUES = 21
BLOCK = 28
HOT_ROWS = 7
OBS = ("z", "y", "c")
PLANE = ("y", "c", "x")
ALL = ("z", "y", "c", "x")
F32 = jnp.float32
BF16 = jnp.bfloat16
VMEM = pl.BlockSpec(memory_space=pltpu.VMEM)
SMEM = pl.BlockSpec(memory_space=pltpu.SMEM)


def two_pieces(x):
    upper = x.astype(BF16).astype(F32)
    return jnp.concatenate([upper, x - upper], axis=0).astype(BF16)


def kept_where(x, row, value):
    rows, lanes = x.shape
    kept = jnp.broadcast_to(row, (16, lanes)) == value
    kept = jnp.where(kept, 1.0, 0.0).astype(BF16)
    return (x.reshape(rows // 16, 16, lanes) * kept[None]).reshape(rows, lanes)


def one_hot(row):
    lanes = row.shape[1]
    spread = lax.broadcasted_iota(jnp.int32, (SPAN, lanes), 0) == row
    return jnp.where(spread, 1.0, 0.0).astype(BF16)


def product(left, right):
    return lax.dot_general(left, right, (((1,), (1,)), ((), ())), preferred_element_type=F32)


def set_operands(left_ref, right_ref, x, ids, parts, at):
    pieces = two_pieces(x)
    rows = pieces.shape[0]
    upper, lower = jnp.right_shift(ids, 8), jnp.bitwise_and(ids, SPAN - 1)
    for part in range(parts):
        left_ref[part * rows : (part + 1) * rows, at : at + LANES] = kept_where(pieces, upper, part)
    right_ref[:, at : at + LANES] = one_hot(lower)


def pack_body(counts_ref, jac_ref, res_ref, cam_ref, out_ref, terms_ref, left_ref, right_ref):
    targets = out_ref.shape[0]
    capacity = jac_ref.shape[1] // targets

    def send(target, hot):
        count = counts_ref[0, target]
        for half in range(2):
            at = pl.multiple_of(target * capacity + half * LANES, LANES)
            here = pl.ds(at, LANES)
            live = lax.broadcasted_iota(jnp.int32, (1, LANES), 1) + half * LANES < count
            row = half * BLOCK
            out_ref[target, row : row + 18, :] = jnp.where(live, jac_ref[:, here], 0.0)
            out_ref[target, row + 18 : row + 20, :] = jnp.where(live, res_ref[:, here], 0.0)
            out_ref[target, row + 20 : row + 21, :] = cam_ref[:, here].astype(F32)
        return jnp.where(count > HALF, target, hot)

    hot = lax.fori_loop(0, targets, send, 0)
    for half in range(2):
        at = pl.multiple_of(hot * capacity + HALF + half * LANES, LANES)
        here = pl.ds(at, LANES)
        count = counts_ref[0, hot]
        live = lax.broadcasted_iota(jnp.int32, (1, LANES), 1) + HALF + half * LANES < count
        jac = jnp.where(live, jac_ref[:, here], 0.0)
        res = jnp.where(live, res_ref[:, here], 0.0)
        ids = cam_ref[:, here]
        first, second = jac[:CAMS], jac[CAMS:]
        for turn in range(5):
            around = first if turn == 0 else jnp.concatenate([first[turn:], first[:turn]], axis=0)
            beside = second if turn == 0 else jnp.concatenate([second[turn:], second[:turn]], axis=0)
            terms_ref[CAMS * turn : CAMS * (turn + 1), :] = first * around + second * beside
        terms_ref[PAIRS : PAIRS + CAMS, :] = first * res[0:1] + second * res[1:2]
        terms_ref[PAIRS + CAMS : TERMS, :] = jnp.zeros((TERMS - PAIRS - CAMS, LANES), F32)
        set_operands(left_ref, right_ref, terms_ref[...], ids, QUARTERS, half * LANES)
    summed = product(left_ref[...], right_ref[...])
    for share in range(targets):
        rows, column = HOT_ROWS * (share // 8), LANES * (share % 8)
        start = 2 * TERMS * (column // SPAN) + rows
        lanes = slice(column % SPAN, column % SPAN + LANES)
        piece = (
            summed[start : start + HOT_ROWS, lanes]
            + summed[start + TERMS : start + TERMS + HOT_ROWS, lanes]
        )
        out_ref[share, VALUES : VALUES + 4, :] = piece[:4]
        out_ref[share, BLOCK + VALUES : BLOCK + VALUES + 3, :] = piece[4:]


def packed(jacobians, residuals, cameras, counts, targets):
    return pl.pallas_call(
        pack_body,
        out_shape=jax.ShapeDtypeStruct((targets, 2 * BLOCK, LANES), F32),
        in_specs=[SMEM, VMEM, VMEM, VMEM],
        out_specs=VMEM,
        scratch_shapes=[
            pltpu.VMEM((TERMS, LANES), F32),
            pltpu.VMEM((2 * TERMS * QUARTERS, 2 * LANES), BF16),
            pltpu.VMEM((SPAN, 2 * LANES), BF16),
        ],
        name="pack",
    )(counts, jacobians, residuals, cameras)


def hot_body(arrived_ref, out_ref):
    arrived = arrived_ref[...]
    out_ref[0:4, :] = arrived[:, VALUES : VALUES + 4, :].sum(axis=0)
    out_ref[4:7, :] = arrived[:, BLOCK + VALUES : BLOCK + VALUES + 3, :].sum(axis=0)


def hot_share(arrived):
    return pl.pallas_call(
        hot_body,
        out_shape=jax.ShapeDtypeStruct((HOT_ROWS, LANES), F32),
        in_specs=[VMEM],
        out_specs=VMEM,
        name="hot",
    )(arrived)


def sums_body(arrived_ref, out_ref, terms_ref, left_ref, right_ref, acc_ref):
    step = pl.program_id(0)

    @pl.when(step == 0)
    def _():
        acc_ref[...] = jnp.zeros_like(acc_ref)
        terms_ref[...] = jnp.zeros_like(terms_ref)

    value = [arrived_ref[pl.ds(row, 8, stride=BLOCK), :] for row in range(VALUES)]
    for turn in range(5):
        for k in range(CAMS):
            other = (k + turn) % CAMS
            term = value[k] * value[other] + value[CAMS + k] * value[CAMS + other]
            terms_ref[pl.ds(CAMS * turn + k, 8, stride=TERMS), :] = term
    for k in range(CAMS):
        term = value[k] * value[18] + value[CAMS + k] * value[19]
        terms_ref[pl.ds(PAIRS + k, 8, stride=TERMS), :] = term
    ids = value[20].astype(jnp.int32)
    for group in range(8):
        x = terms_ref[group * TERMS : (group + 1) * TERMS, :]
        row = ids[group : group + 1, :]
        set_operands(left_ref, right_ref, x, row, QUARTERS, group * LANES)
    acc_ref[...] += product(left_ref[...], right_ref[...])

    @pl.when(step == pl.num_programs(0) - 1)
    def _():
        for part in range(QUARTERS):
            at = 2 * TERMS * part
            out_ref[part] = acc_ref[at : at + TERMS, :] + acc_ref[at + TERMS : at + 2 * TERMS, :]


def camera_sums(arrived):
    rows = arrived.shape[0]
    depth = 8 * LANES
    return pl.pallas_call(
        sums_body,
        grid=(rows // (8 * BLOCK),),
        out_shape=jax.ShapeDtypeStruct((QUARTERS, TERMS, SPAN), F32),
        in_specs=[pl.BlockSpec((8 * BLOCK, LANES), lambda i: (i, 0))],
        out_specs=pl.BlockSpec((QUARTERS, TERMS, SPAN), lambda i: (0, 0, 0)),
        scratch_shapes=[
            pltpu.VMEM((8 * TERMS, LANES), F32),
            pltpu.VMEM((2 * TERMS * QUARTERS, depth), BF16),
            pltpu.VMEM((SPAN, depth), BF16),
            pltpu.VMEM((2 * TERMS * QUARTERS, SPAN), F32),
        ],
        cost_estimate=pl.CostEstimate(
            flops=2 * 2 * TERMS * CAM_DEV * 128 * rows // BLOCK, transcendentals=0, bytes_accessed=rows * 512
        ),
        name="sums",
    )(arrived)


def add_body(own_ref, summed_ref, hot_ref, out_ref):
    own = own_ref[0, 0]
    for part in range(QUARTERS):
        for share in range(2):
            for group in range(8):
                rows = slice(HOT_ROWS * group, HOT_ROWS * (group + 1))
                lanes = slice(share * LANES, (share + 1) * LANES)
                piece = jnp.where(own > 0, hot_ref[group * 8 + part * 2 + share], 0.0)
                out_ref[part, rows, lanes] = summed_ref[part, rows, lanes] + piece


def with_hot(summed, hot, own):
    return pl.pallas_call(
        add_body,
        out_shape=jax.ShapeDtypeStruct(summed.shape, F32),
        in_specs=[SMEM, VMEM, VMEM],
        out_specs=VMEM,
        name="add",
    )(own, summed, hot)


def place_body(first_ref, slots_ref, ids_ref, out_ref, left_ref, right_ref, acc_ref):
    sources = slots_ref.shape[0]
    ranges = out_ref.shape[0]
    first = first_ref[0, 0]
    acc_ref[...] = jnp.zeros_like(acc_ref)

    def add(step, carry):
        for inner in range(4):
            source = step * 4 + inner
            for half in range(2):
                x = slots_ref[source, half * CAMS : (half + 1) * CAMS, :]
                x = jnp.concatenate([x, jnp.zeros((16 - CAMS, LANES), F32)], axis=0)
                ids = ids_ref[source, half : half + 1, :] - first
                at = (inner * 2 + half) * LANES
                set_operands(left_ref, right_ref, x, ids, ranges, at)
        acc_ref[...] += product(left_ref[...], right_ref[...])
        return carry

    lax.fori_loop(0, sources // 4, add, 0)
    for part in range(ranges):
        at = 32 * part
        both = acc_ref[at : at + CAMS, :] + acc_ref[at + 16 : at + 16 + CAMS, :]
        out_ref[part, :CAMS, :] = both[:, :LANES]
        out_ref[part, CAMS:, :] = both[:, LANES:]


def placed(slots, ids, first, ranges):
    depth = 8 * LANES
    return pl.pallas_call(
        place_body,
        out_shape=jax.ShapeDtypeStruct((ranges, 2 * CAMS, LANES), F32),
        in_specs=[SMEM, VMEM, VMEM],
        out_specs=VMEM,
        scratch_shapes=[
            pltpu.VMEM((32 * ranges, depth), BF16),
            pltpu.VMEM((SPAN, depth), BF16),
            pltpu.VMEM((32 * ranges, SPAN), F32),
        ],
        name="place",
    )(first, slots, ids)


def blocks_body(shares_ref, out_ref):
    for k in range(CAMS):
        for l in range(CAMS):
            ahead, behind = (l - k) % CAMS, (k - l) % CAMS
            row = CAMS * ahead + k if ahead <= 4 else CAMS * behind + l
            for part in range(QUARTERS):
                lanes = slice(part * SPAN, (part + 1) * SPAN)
                at = k * CAMS + l
                out_ref[at : at + 1, lanes] = shares_ref[part, row : row + 1, :]


def whole_blocks(shares):
    return pl.pallas_call(
        blocks_body,
        out_shape=jax.ShapeDtypeStruct((CAMS * CAMS, CAM_DEV), F32),
        in_specs=[VMEM],
        out_specs=VMEM,
        name="blocks",
    )(shares)


def order_body(rows_ref, out_ref):
    groups = rows_ref.shape[0] // (16 * CAMS)
    for ends in range(groups):
        x, y, c = ends % 4, ends // 4 % 4, ends // 16
        for tile in range(16):
            source = (ends * 16 + tile) * CAMS
            at = (((y * 2 + c) * 4 + x) * 16 + tile) * LANES
            out_ref[:, at : at + LANES] = rows_ref[source : source + CAMS, :]


def ordered(rows):
    return pl.pallas_call(
        order_body,
        out_shape=jax.ShapeDtypeStruct((CAMS, rows.shape[0] // CAMS * LANES), F32),
        in_specs=[VMEM],
        out_specs=VMEM,
        name="order",
    )(rows)


def exchanged(pieces, axes):
    return lax.all_to_all(pieces, axes, 0, 0, tiled=True)


def from_all(share, axes):
    count = lax.axis_size(axes)
    return exchanged(jnp.broadcast_to(share[None], (count, *share.shape)), axes)


def local(jacobians, residuals, camera_local, bucket_counts, camera_map):
    targets = lax.axis_size(OBS)
    levels = lax.axis_size("z")
    cameras = camera_local.reshape(1, -1)
    sent = packed(jacobians, residuals, cameras, bucket_counts, targets)
    arrived = exchanged(sent, OBS)
    hot = from_all(hot_share(arrived), OBS)
    summed = camera_sums(arrived.reshape(targets * 2 * BLOCK, LANES))
    own = jnp.argmax(bucket_counts[0]) == lax.axis_index(OBS)
    summed = with_hot(summed, hot, own.astype(jnp.int32).reshape(1, 1))
    share = exchanged(summed, "x").sum(axis=0)
    blocks = whole_blocks(from_all(share[:48], "x"))
    slots = share[PAIRS : PAIRS + CAMS]
    slots = jnp.concatenate([slots[:, :LANES], slots[:, LANES:]], axis=0)
    slots = from_all(slots, PLANE)
    plane = slots.shape[0] * SPAN
    ids = lax.dynamic_slice_in_dim(camera_map, lax.axis_index("z") * plane, plane)
    first = lax.axis_index(PLANE) * levels * SPAN
    part = placed(slots, ids.reshape(-1, 2, LANES), first.reshape(1, 1), levels)
    part = exchanged(part, "z").sum(axis=0)
    part = from_all(part, "z")
    part = from_all(part.reshape(-1, LANES), ("y", "x"))
    part = from_all(part.reshape(-1, LANES), "c")
    gradient = ordered(part.reshape(-1, LANES))
    return gradient, blocks


def solution(mesh):
    split = Mesh(mesh.devices.reshape(8, 4, 2, mesh.shape["rep"]), ALL)
    return jax.shard_map(
        local,
        mesh=split,
        in_specs=(P(None, ALL), P(None, ALL), P(ALL), P(ALL, None), P()),
        out_specs=(P(), P(None, OBS)),
        check_vma=False,
    )
```

```python
import jax
import jax.numpy as jnp
from jax import lax
from jax.experimental import pallas as pl
from jax.experimental.pallas import tpu as pltpu
from jax.sharding import Mesh
from jax.sharding import PartitionSpec as P

CAM_DEV = 1024
HALF = 256
LANES = 128
SPAN = 256
QUARTERS = CAM_DEV // SPAN
CAMS = 9
PAIRS = 45
TERMS = 56
VALUES = 21
BLOCK = 26
HOT_ROWS = 14
SHARE_ROWS = 128
OBS = ("z", "y", "c")
PLANE = ("y", "c", "x")
ALL = ("z", "y", "c", "x")
F32 = jnp.float32
BF16 = jnp.bfloat16
VMEM = pl.BlockSpec(memory_space=pltpu.VMEM)
SMEM = pl.BlockSpec(memory_space=pltpu.SMEM)


def two_pieces(x):
    upper = x.astype(BF16).astype(F32)
    return jnp.concatenate([upper, x - upper], axis=0).astype(BF16)


def kept_where(x, row, value):
    rows, lanes = x.shape
    kept = jnp.broadcast_to(row, (16, lanes)) == value
    kept = jnp.where(kept, 1.0, 0.0).astype(BF16)
    return (x.reshape(rows // 16, 16, lanes) * kept[None]).reshape(rows, lanes)


def one_hot(row):
    lanes = row.shape[1]
    spread = lax.broadcasted_iota(jnp.int32, (SPAN, lanes), 0) == row
    return jnp.where(spread, 1.0, 0.0).astype(BF16)


def product(left, right):
    return lax.dot_general(left, right, (((1,), (1,)), ((), ())), preferred_element_type=F32)


def set_operands(left_ref, right_ref, x, ids, parts, at):
    pieces = two_pieces(x)
    rows = pieces.shape[0]
    upper, lower = jnp.right_shift(ids, 8), jnp.bitwise_and(ids, SPAN - 1)
    for part in range(parts):
        left_ref[part * rows : (part + 1) * rows, at : at + LANES] = kept_where(pieces, upper, part)
    right_ref[:, at : at + LANES] = one_hot(lower)


def hot_piece(block):
    return slice(4 * block, min(4 * block + 4, HOT_ROWS))


def pack_body(counts_ref, jac_ref, res_ref, cam_ref, out_ref, terms_ref, left_ref, right_ref):
    targets = out_ref.shape[0]
    capacity = jac_ref.shape[1] // (2 * targets)

    def send(target, hot):
        for side in range(2):
            bucket = (2 * lax.rem(target, 4) + side) * 8 + lax.div(target, 4)
            count = counts_ref[0, bucket]
            for half in range(2):
                at = pl.multiple_of(bucket * capacity + half * LANES, LANES)
                here = pl.ds(at, LANES)
                live = lax.broadcasted_iota(jnp.int32, (1, LANES), 1) + half * LANES < count
                row = (2 * side + half) * BLOCK
                out_ref[target, row : row + 18, :] = jnp.where(live, jac_ref[:, here], 0.0)
                out_ref[target, row + 18 : row + 20, :] = jnp.where(live, res_ref[:, here], 0.0)
                out_ref[target, row + 20 : row + 21, :] = cam_ref[:, here].astype(F32)
            hot = jnp.where(count > HALF, bucket, hot)
        return hot

    hot = lax.fori_loop(0, targets, send, 0)
    for half in range(2):
        at = pl.multiple_of(hot * capacity + HALF + half * LANES, LANES)
        here = pl.ds(at, LANES)
        count = counts_ref[0, hot]
        live = lax.broadcasted_iota(jnp.int32, (1, LANES), 1) + HALF + half * LANES < count
        jac = jnp.where(live, jac_ref[:, here], 0.0)
        res = jnp.where(live, res_ref[:, here], 0.0)
        ids = cam_ref[:, here]
        first, second = jac[:CAMS], jac[CAMS:]
        for turn in range(5):
            around = first if turn == 0 else jnp.concatenate([first[turn:], first[:turn]], axis=0)
            beside = second if turn == 0 else jnp.concatenate([second[turn:], second[:turn]], axis=0)
            terms_ref[CAMS * turn : CAMS * (turn + 1), :] = first * around + second * beside
        terms_ref[PAIRS : PAIRS + CAMS, :] = first * res[0:1] + second * res[1:2]
        terms_ref[PAIRS + CAMS : TERMS, :] = jnp.zeros((TERMS - PAIRS - CAMS, LANES), F32)
        set_operands(left_ref, right_ref, terms_ref[...], ids, QUARTERS, half * LANES)
    summed = product(left_ref[...], right_ref[...])
    for share in range(targets):
        rows, column = HOT_ROWS * (share // 8), LANES * (share % 8)
        start = 2 * TERMS * (column // SPAN) + rows
        lanes = slice(column % SPAN, column % SPAN + LANES)
        piece = (
            summed[start : start + HOT_ROWS, lanes]
            + summed[start + TERMS : start + TERMS + HOT_ROWS, lanes]
        )
        for block in range(4):
            part = piece[hot_piece(block)]
            row = block * BLOCK + VALUES
            out_ref[share, row : row + part.shape[0], :] = part


def packed(jacobians, residuals, cameras, counts, targets):
    return pl.pallas_call(
        pack_body,
        out_shape=jax.ShapeDtypeStruct((targets, 4 * BLOCK, LANES), F32),
        in_specs=[SMEM, VMEM, VMEM, VMEM],
        out_specs=VMEM,
        scratch_shapes=[
            pltpu.VMEM((TERMS, LANES), F32),
            pltpu.VMEM((2 * TERMS * QUARTERS, 2 * LANES), BF16),
            pltpu.VMEM((SPAN, 2 * LANES), BF16),
        ],
        name="pack",
    )(counts, jacobians, residuals, cameras)


def sums_body(arrived_ref, out_ref, terms_ref, left_ref, right_ref, acc_ref, hot_ref):
    step = pl.program_id(0)

    @pl.when(step == 0)
    def _():
        acc_ref[...] = jnp.zeros_like(acc_ref)
        terms_ref[...] = jnp.zeros_like(terms_ref)
        hot_ref[...] = jnp.zeros_like(hot_ref)

    for pair in range(2):
        start = pair * 8 * BLOCK
        value = [arrived_ref[pl.ds(start + row, 8, stride=BLOCK), :] for row in range(VALUES)]
        for turn in range(5):
            for k in range(CAMS):
                other = (k + turn) % CAMS
                term = value[k] * value[other] + value[CAMS + k] * value[CAMS + other]
                terms_ref[pair, pl.ds(CAMS * turn + k, 8, stride=TERMS), :] = term
        for k in range(CAMS):
            term = value[k] * value[18] + value[CAMS + k] * value[19]
            terms_ref[pair, pl.ds(PAIRS + k, 8, stride=TERMS), :] = term
        ids = value[20].astype(jnp.int32)
        for group in range(8):
            x = terms_ref[pair, group * TERMS : (group + 1) * TERMS, :]
            side, half = group % 4 // 2, group % 2
            at = ((pair * 2 + group // 4) * 2 + half) * LANES
            row = ids[group : group + 1, :]
            set_operands(left_ref.at[side], right_ref.at[side], x, row, QUARTERS, at)
    for source in range(4):
        for block in range(4):
            part = hot_piece(block)
            row = (source * 4 + block) * BLOCK + VALUES
            hot_ref[part, :] += arrived_ref[row : row + part.stop - part.start, :]
    for side in range(2):
        acc_ref[side] += product(left_ref[side], right_ref[side])

    @pl.when(step == pl.num_programs(0) - 1)
    def _():
        for side in range(2):
            for part in range(QUARTERS):
                at = 2 * TERMS * part
                both = acc_ref[side, at : at + TERMS, :] + acc_ref[side, at + TERMS : at + 2 * TERMS, :]
                level = side * QUARTERS + part
                out_ref[level, :TERMS, :] = both[:, :LANES]
                out_ref[level, TERMS : 2 * TERMS, :] = both[:, LANES:]
                out_ref[level, 2 * TERMS :, :] = hot_ref[...]


def camera_sums(arrived):
    rows = arrived.shape[0]
    depth = 8 * LANES
    out = (2 * QUARTERS, SHARE_ROWS, LANES)
    return pl.pallas_call(
        sums_body,
        grid=(rows // (16 * BLOCK),),
        out_shape=jax.ShapeDtypeStruct(out, F32),
        in_specs=[pl.BlockSpec((16 * BLOCK, LANES), lambda i: (i, 0))],
        out_specs=pl.BlockSpec(out, lambda i: (0, 0, 0)),
        scratch_shapes=[
            pltpu.VMEM((2, 8 * TERMS, LANES), F32),
            pltpu.VMEM((2, 2 * TERMS * QUARTERS, depth), BF16),
            pltpu.VMEM((2, SPAN, depth), BF16),
            pltpu.VMEM((2, 2 * TERMS * QUARTERS, SPAN), F32),
            pltpu.VMEM((SHARE_ROWS - 2 * TERMS, LANES), F32),
        ],
        cost_estimate=pl.CostEstimate(
            flops=2 * 2 * TERMS * CAM_DEV * 128 * rows // BLOCK, transcendentals=0, bytes_accessed=rows * 512
        ),
        name="sums",
    )(arrived)


def place_body(first_ref, slots_ref, ids_ref, out_ref, left_ref, right_ref, acc_ref):
    sources = slots_ref.shape[0]
    ranges = out_ref.shape[0]
    first = first_ref[0, 0]
    acc_ref[...] = jnp.zeros_like(acc_ref)

    def set_group(x, ids, group):
        x = jnp.concatenate([x, jnp.zeros((16 - CAMS, LANES), F32)], axis=0)
        set_operands(left_ref, right_ref, x, ids - first, ranges, group * LANES)

    def add(step, carry):
        for group in range(8):
            source, half = step * 4 + group // 2, group % 2
            x = slots_ref[source, half * CAMS : (half + 1) * CAMS, :]
            set_group(x, ids_ref[source, half : half + 1, :], group)
        acc_ref[...] += product(left_ref[...], right_ref[...])
        return carry

    lax.fori_loop(0, sources // 4, add, 0)
    row = 2 * CAMS + PAIRS % HOT_ROWS
    for group in range(8):
        x = slots_ref[PAIRS // HOT_ROWS * 8 + group, row : row + CAMS, :]
        set_group(x, ids_ref[sources + group // 2, group % 2 : group % 2 + 1, :], group)
    acc_ref[...] += product(left_ref[...], right_ref[...])
    for part in range(ranges):
        at = 32 * part
        both = acc_ref[at : at + CAMS, :] + acc_ref[at + 16 : at + 16 + CAMS, :]
        out_ref[part, :CAMS, :] = both[:, :LANES]
        out_ref[part, CAMS:, :] = both[:, LANES:]


def placed(slots, ids, first, ranges):
    depth = 8 * LANES
    return pl.pallas_call(
        place_body,
        out_shape=jax.ShapeDtypeStruct((ranges, 2 * CAMS, LANES), F32),
        in_specs=[SMEM, VMEM, VMEM],
        out_specs=VMEM,
        scratch_shapes=[
            pltpu.VMEM((32 * ranges, depth), BF16),
            pltpu.VMEM((SPAN, depth), BF16),
            pltpu.VMEM((32 * ranges, SPAN), F32),
        ],
        name="place",
    )(first, slots, ids)


def blocks_body(place_ref, one_ref, two_ref, three_ref, four_ref, slots_ref, out_ref, rows_ref):
    column, own = place_ref[0, 0], place_ref[0, 1]
    for turn, share_ref in enumerate((one_ref, two_ref, three_ref, four_ref)):
        part = lax.rem(column - turn + QUARTERS, QUARTERS)
        for half in range(2):
            for group in range(4):
                at = HOT_ROWS * group
                hot = slots_ref[group * 8 + part * 2 + half, 2 * CAMS : 2 * CAMS + HOT_ROWS, :]
                share = share_ref[half * TERMS + at : half * TERMS + at + HOT_ROWS, :]
                rows_ref[at : at + HOT_ROWS, :] = share + jnp.where(own > 0, hot, 0.0)
            lanes = pl.ds(pl.multiple_of((part * 2 + half) * LANES, LANES), LANES)
            for k in range(CAMS):
                for l in range(CAMS):
                    ahead, behind = (l - k) % CAMS, (k - l) % CAMS
                    row = CAMS * ahead + k if ahead <= 4 else CAMS * behind + l
                    at = k * CAMS + l
                    out_ref[at : at + 1, lanes] = rows_ref[row : row + 1, :]


def whole_blocks(place, shares, slots):
    return pl.pallas_call(
        blocks_body,
        out_shape=jax.ShapeDtypeStruct((CAMS * CAMS, CAM_DEV), F32),
        in_specs=[SMEM] + [VMEM] * 5,
        out_specs=VMEM,
        scratch_shapes=[pltpu.VMEM((TERMS, LANES), F32)],
        name="blocks",
    )(place, *shares, slots)


def order_body(core_ref, own_ref, other_ref, out_ref):
    for turn, rows_ref in enumerate((own_ref, other_ref)):
        core = jnp.bitwise_xor(core_ref[0, 0], turn)
        for ends in range(rows_ref.shape[0] // (16 * CAMS)):
            x, y = ends % 4, ends // 4
            for tile in range(16):
                source = (ends * 16 + tile) * CAMS
                at = pl.multiple_of((((y * 2 + core) * 4 + x) * 16 + tile) * LANES, LANES)
                out_ref[:, pl.ds(at, LANES)] = rows_ref[source : source + CAMS, :]


def ordered(core, own, other):
    return pl.pallas_call(
        order_body,
        out_shape=jax.ShapeDtypeStruct((CAMS, 2 * own.shape[0] // CAMS * LANES), F32),
        in_specs=[SMEM, VMEM, VMEM],
        out_specs=VMEM,
        name="order",
    )(core, own, other)


def exchanged(pieces, axes):
    return lax.all_to_all(pieces, axes, 0, 0, tiled=True)


def from_all(share, axes):
    count = lax.axis_size(axes)
    return exchanged(jnp.broadcast_to(share[None], (count, *share.shape)), axes)


def to_owner(share, turn):
    pairs = []
    for level in range(8):
        for column in range(4):
            target = (2 * column + level // 4) * 4 + (level % 4 + turn) % 4
            pairs.append((level * 4 + column, target))
    return lax.ppermute(share, ("z", "x"), pairs)


def local(jacobians, residuals, camera_local, bucket_counts, camera_map):
    targets = lax.axis_size(PLANE)
    levels = lax.axis_size("z")
    level, core = lax.axis_index("z"), lax.axis_index("c")
    hot = jnp.argmax(bucket_counts[0])
    ids = camera_map.reshape(4, 2, 4, 2, QUARTERS, SPAN)
    ids = lax.dynamic_slice(ids, (0, level // 4, 0, 0, level % 4, 0), (4, 1, 4, 2, 1, SPAN))
    ids = ids.reshape(4, 4, 2, SPAN).transpose(1, 2, 0, 3).reshape(targets, 2, LANES)
    hot_ids = lax.dynamic_slice_in_dim(camera_map, hot * CAM_DEV, CAM_DEV)
    hot_ids = jnp.where(level == 0, hot_ids, -1).reshape(-1, 2, LANES)
    ids = jnp.concatenate([ids, hot_ids], axis=0)

    cameras = camera_local.reshape(1, -1)
    sent = packed(jacobians, residuals, cameras, bucket_counts, targets)
    arrived = exchanged(sent, PLANE)
    summed = camera_sums(arrived.reshape(-1, LANES))
    share = exchanged(summed, "z").sum(axis=0)
    shares = [to_owner(share[: 2 * TERMS], turn) for turn in range(4)]
    slots = [share[PAIRS : PAIRS + CAMS], share[TERMS + PAIRS : TERMS + PAIRS + CAMS]]
    slots.append(share[2 * TERMS : 2 * TERMS + HOT_ROWS])
    slots = from_all(jnp.concatenate(slots, axis=0), PLANE)
    own = (hot == lax.axis_index(OBS)).astype(jnp.int32)
    blocks = whole_blocks(jnp.stack([lax.axis_index("x"), own]).reshape(1, 2), shares, slots)
    first = lax.axis_index(PLANE) * levels * SPAN
    part = placed(slots, ids, first.reshape(1, 1), levels)
    part = exchanged(part, "z").sum(axis=0)
    part = from_all(part, "z")
    part = from_all(part.reshape(-1, LANES), ("y", "x")).reshape(-1, LANES)
    other = lax.ppermute(part, "c", [(0, 1), (1, 0)])
    gradient = ordered(core.reshape(1, 1), part, other)
    return gradient, blocks


def solution(mesh):
    split = Mesh(mesh.devices.reshape(8, 4, 2, mesh.shape["rep"]), ALL)
    return jax.shard_map(
        local,
        mesh=split,
        in_specs=(P(None, ALL), P(None, ALL), P(ALL), P(ALL, None), P()),
        out_specs=(P(), P(None, OBS)),
        check_vma=False,
    )
```

```python
import jax
import jax.numpy as jnp
from jax import lax
from jax.experimental import pallas as pl
from jax.experimental.pallas import tpu as pltpu
from jax.sharding import Mesh
from jax.sharding import PartitionSpec as P

CAM_DEV = 1024
HALF = 256
LANES = 128
SPAN = 256
QUARTERS = CAM_DEV // SPAN
CAMS = 9
PAIRS = 45
TERMS = 56
VALUES = 21
BLOCK = 26
HOT_ROWS = 14
EXTRA_ROWS = 16
GRAD_ROWS = 2 * CAMS + HOT_ROWS
BLOCK_ROWS = 48
OBS = ("z", "y", "c")
PLANE = ("y", "c", "x")
ALL = ("z", "y", "c", "x")
F32 = jnp.float32
BF16 = jnp.bfloat16
VMEM = pl.BlockSpec(memory_space=pltpu.VMEM)
SMEM = pl.BlockSpec(memory_space=pltpu.SMEM)


def two_pieces(x):
    upper = x.astype(BF16).astype(F32)
    return jnp.concatenate([upper, x - upper], axis=0).astype(BF16)


def kept_where(x, row, value):
    rows, lanes = x.shape
    kept = jnp.broadcast_to(row, (16, lanes)) == value
    kept = jnp.where(kept, 1.0, 0.0).astype(BF16)
    return (x.reshape(rows // 16, 16, lanes) * kept[None]).reshape(rows, lanes)


def one_hot(row):
    lanes = row.shape[1]
    spread = lax.broadcasted_iota(jnp.int32, (SPAN, lanes), 0) == row
    return jnp.where(spread, 1.0, 0.0).astype(BF16)


def product(left, right):
    return lax.dot_general(left, right, (((1,), (1,)), ((), ())), preferred_element_type=F32)


def set_operands(left_ref, right_ref, x, ids, parts, at):
    pieces = two_pieces(x)
    rows = pieces.shape[0]
    upper, lower = jnp.right_shift(ids, 8), jnp.bitwise_and(ids, SPAN - 1)
    for part in range(parts):
        left_ref[part * rows : (part + 1) * rows, at : at + LANES] = kept_where(pieces, upper, part)
    right_ref[:, at : at + LANES] = one_hot(lower)


def hot_piece(block):
    return slice(4 * block, min(4 * block + 4, HOT_ROWS))


def pack_body(counts_ref, jac_ref, res_ref, cam_ref, out_ref, terms_ref, left_ref, right_ref):
    targets = out_ref.shape[0]
    capacity = jac_ref.shape[1] // (2 * targets)

    def send(target, hot):
        for side in range(2):
            bucket = (2 * lax.rem(target, 4) + side) * 8 + lax.div(target, 4)
            count = counts_ref[0, bucket]
            for half in range(2):
                at = pl.multiple_of(bucket * capacity + half * LANES, LANES)
                here = pl.ds(at, LANES)
                live = lax.broadcasted_iota(jnp.int32, (1, LANES), 1) + half * LANES < count
                row = (2 * side + half) * BLOCK
                out_ref[target, row : row + 18, :] = jnp.where(live, jac_ref[:, here], 0.0)
                out_ref[target, row + 18 : row + 20, :] = jnp.where(live, res_ref[:, here], 0.0)
                out_ref[target, row + 20 : row + 21, :] = cam_ref[:, here].astype(F32)
            hot = jnp.where(count > HALF, bucket, hot)
        return hot

    hot = lax.fori_loop(0, targets, send, 0)
    for half in range(2):
        at = pl.multiple_of(hot * capacity + HALF + half * LANES, LANES)
        here = pl.ds(at, LANES)
        count = counts_ref[0, hot]
        live = lax.broadcasted_iota(jnp.int32, (1, LANES), 1) + HALF + half * LANES < count
        jac = jnp.where(live, jac_ref[:, here], 0.0)
        res = jnp.where(live, res_ref[:, here], 0.0)
        ids = cam_ref[:, here]
        first, second = jac[:CAMS], jac[CAMS:]
        for turn in range(5):
            around = first if turn == 0 else jnp.concatenate([first[turn:], first[:turn]], axis=0)
            beside = second if turn == 0 else jnp.concatenate([second[turn:], second[:turn]], axis=0)
            terms_ref[CAMS * turn : CAMS * (turn + 1), :] = first * around + second * beside
        terms_ref[PAIRS : PAIRS + CAMS, :] = first * res[0:1] + second * res[1:2]
        terms_ref[PAIRS + CAMS : TERMS, :] = jnp.zeros((TERMS - PAIRS - CAMS, LANES), F32)
        set_operands(left_ref, right_ref, terms_ref[...], ids, QUARTERS, half * LANES)
    summed = product(left_ref[...], right_ref[...])
    for share in range(targets):
        rows, column = HOT_ROWS * (share // 8), LANES * (share % 8)
        start = 2 * TERMS * (column // SPAN) + rows
        lanes = slice(column % SPAN, column % SPAN + LANES)
        piece = (
            summed[start : start + HOT_ROWS, lanes]
            + summed[start + TERMS : start + TERMS + HOT_ROWS, lanes]
        )
        for block in range(4):
            part = piece[hot_piece(block)]
            row = block * BLOCK + VALUES
            out_ref[share, row : row + part.shape[0], :] = part


def packed(jacobians, residuals, cameras, counts, targets):
    return pl.pallas_call(
        pack_body,
        out_shape=jax.ShapeDtypeStruct((targets, 4 * BLOCK, LANES), F32),
        in_specs=[SMEM, VMEM, VMEM, VMEM],
        out_specs=VMEM,
        scratch_shapes=[
            pltpu.VMEM((TERMS, LANES), F32),
            pltpu.VMEM((2 * TERMS * QUARTERS, 2 * LANES), BF16),
            pltpu.VMEM((SPAN, 2 * LANES), BF16),
        ],
        name="pack",
    )(counts, jacobians, residuals, cameras)


def sums_body(arrived_ref, out_ref, terms_ref, left_ref, right_ref, acc_ref, hot_ref):
    step = pl.program_id(0)

    @pl.when(step == 0)
    def _():
        acc_ref[...] = jnp.zeros_like(acc_ref)
        terms_ref[...] = jnp.zeros_like(terms_ref)
        hot_ref[...] = jnp.zeros_like(hot_ref)

    for pair in range(2):
        start = pair * 8 * BLOCK
        value = [arrived_ref[pl.ds(start + row, 8, stride=BLOCK), :] for row in range(VALUES)]
        for turn in range(5):
            for k in range(CAMS):
                other = (k + turn) % CAMS
                term = value[k] * value[other] + value[CAMS + k] * value[CAMS + other]
                terms_ref[pair, pl.ds(CAMS * turn + k, 8, stride=TERMS), :] = term
        for k in range(CAMS):
            term = value[k] * value[18] + value[CAMS + k] * value[19]
            terms_ref[pair, pl.ds(PAIRS + k, 8, stride=TERMS), :] = term
        ids = value[20].astype(jnp.int32)
        for group in range(8):
            x = terms_ref[pair, group * TERMS : (group + 1) * TERMS, :]
            side, half = group % 4 // 2, group % 2
            at = ((pair * 2 + group // 4) * 2 + half) * LANES
            row = ids[group : group + 1, :]
            set_operands(left_ref.at[side], right_ref.at[side], x, row, QUARTERS, at)
    for source in range(4):
        for block in range(4):
            part = hot_piece(block)
            row = (source * 4 + block) * BLOCK + VALUES
            hot_ref[part, :] += arrived_ref[row : row + part.stop - part.start, :]
    for side in range(2):
        acc_ref[side] += product(left_ref[side], right_ref[side])

    @pl.when(step == pl.num_programs(0) - 1)
    def _():
        for side in range(2):
            for part in range(QUARTERS):
                at = 2 * TERMS * part
                both = acc_ref[side, at : at + TERMS, :] + acc_ref[side, at + TERMS : at + 2 * TERMS, :]
                level = side * QUARTERS + part
                for half in range(2):
                    lanes = slice(half * LANES, (half + 1) * LANES)
                    at = GRAD_ROWS + half * BLOCK_ROWS
                    out_ref[level, at : at + BLOCK_ROWS, :] = both[:BLOCK_ROWS, lanes]
                    out_ref[level, half * CAMS : (half + 1) * CAMS, :] = both[PAIRS : PAIRS + CAMS, lanes]
                out_ref[level, 2 * CAMS : GRAD_ROWS, :] = hot_ref[:HOT_ROWS]


def camera_sums(arrived):
    rows = arrived.shape[0]
    depth = 8 * LANES
    out = (2 * QUARTERS, GRAD_ROWS + 2 * BLOCK_ROWS, LANES)
    return pl.pallas_call(
        sums_body,
        grid=(rows // (16 * BLOCK),),
        out_shape=jax.ShapeDtypeStruct(out, F32),
        in_specs=[pl.BlockSpec((16 * BLOCK, LANES), lambda i: (i, 0))],
        out_specs=pl.BlockSpec(out, lambda i: (0, 0, 0)),
        scratch_shapes=[
            pltpu.VMEM((2, 8 * TERMS, LANES), F32),
            pltpu.VMEM((2, 2 * TERMS * QUARTERS, depth), BF16),
            pltpu.VMEM((2, SPAN, depth), BF16),
            pltpu.VMEM((2, 2 * TERMS * QUARTERS, SPAN), F32),
            pltpu.VMEM((EXTRA_ROWS, LANES), F32),
        ],
        cost_estimate=pl.CostEstimate(
            flops=2 * 2 * TERMS * CAM_DEV * 128 * rows // BLOCK, transcendentals=0, bytes_accessed=rows * 512
        ),
        name="sums",
    )(arrived)


def place_body(first_ref, slots_ref, ids_ref, out_ref, left_ref, right_ref, acc_ref):
    sources = slots_ref.shape[0]
    ranges = out_ref.shape[0]
    first = first_ref[0, 0]
    acc_ref[...] = jnp.zeros_like(acc_ref)

    def set_group(x, ids, group):
        x = jnp.concatenate([x, jnp.zeros((16 - CAMS, LANES), F32)], axis=0)
        set_operands(left_ref, right_ref, x, ids - first, ranges, group * LANES)

    def add(step, carry):
        for group in range(8):
            source, half = step * 4 + group // 2, group % 2
            x = slots_ref[source, half * CAMS : (half + 1) * CAMS, :]
            set_group(x, ids_ref[source, half : half + 1, :], group)
        acc_ref[...] += product(left_ref[...], right_ref[...])
        return carry

    lax.fori_loop(0, sources // 4, add, 0)
    row = 2 * CAMS + PAIRS % HOT_ROWS
    for group in range(8):
        x = slots_ref[PAIRS // HOT_ROWS * 8 + group, row : row + CAMS, :]
        set_group(x, ids_ref[sources + group // 2, group % 2 : group % 2 + 1, :], group)
    acc_ref[...] += product(left_ref[...], right_ref[...])
    for part in range(ranges):
        at = 32 * part
        both = acc_ref[at : at + CAMS, :] + acc_ref[at + 16 : at + 16 + CAMS, :]
        out_ref[part, :CAMS, :] = both[:, :LANES]
        out_ref[part, CAMS:, :] = both[:, LANES:]


def placed(slots, ids, first, ranges):
    depth = 8 * LANES
    return pl.pallas_call(
        place_body,
        out_shape=jax.ShapeDtypeStruct((ranges, 2 * CAMS, LANES), F32),
        in_specs=[SMEM, VMEM, VMEM],
        out_specs=VMEM,
        scratch_shapes=[
            pltpu.VMEM((32 * ranges, depth), BF16),
            pltpu.VMEM((SPAN, depth), BF16),
            pltpu.VMEM((32 * ranges, SPAN), F32),
        ],
        name="place",
    )(first, slots, ids)


def blocks_body(place_ref, one_ref, two_ref, three_ref, four_ref, slots_ref, out_ref, rows_ref):
    column, own = place_ref[0, 0], place_ref[0, 1]
    for turn, share_ref in enumerate((one_ref, two_ref, three_ref, four_ref)):
        part = lax.rem(column - turn + QUARTERS, QUARTERS)
        for half in range(2):
            for group in range(4):
                start, stop = HOT_ROWS * group, min(HOT_ROWS * (group + 1), PAIRS)
                hot = slots_ref[group * 8 + part * 2 + half, 2 * CAMS : 2 * CAMS + stop - start, :]
                share = share_ref[half * BLOCK_ROWS + start : half * BLOCK_ROWS + stop, :]
                rows_ref[start:stop, :] = share + jnp.where(own > 0, hot, 0.0)
            lanes = pl.ds(pl.multiple_of((part * 2 + half) * LANES, LANES), LANES)
            for k in range(CAMS):
                for l in range(CAMS):
                    ahead, behind = (l - k) % CAMS, (k - l) % CAMS
                    row = CAMS * ahead + k if ahead <= 4 else CAMS * behind + l
                    at = k * CAMS + l
                    out_ref[at : at + 1, lanes] = rows_ref[row : row + 1, :]


def whole_blocks(place, shares, slots):
    return pl.pallas_call(
        blocks_body,
        out_shape=jax.ShapeDtypeStruct((CAMS * CAMS, CAM_DEV), F32),
        in_specs=[SMEM] + [VMEM] * 5,
        out_specs=VMEM,
        scratch_shapes=[pltpu.VMEM((BLOCK_ROWS, LANES), F32)],
        name="blocks",
    )(place, *shares, slots)


def order_body(core_ref, own_ref, other_ref, out_ref):
    for turn, rows_ref in enumerate((own_ref, other_ref)):
        core = jnp.bitwise_xor(core_ref[0, 0], turn)
        for ends in range(rows_ref.shape[0] // (16 * CAMS)):
            x, y = ends % 4, ends // 4
            for tile in range(16):
                source = (ends * 16 + tile) * CAMS
                at = pl.multiple_of((((y * 2 + core) * 4 + x) * 16 + tile) * LANES, LANES)
                out_ref[:, pl.ds(at, LANES)] = rows_ref[source : source + CAMS, :]


def ordered(core, own, other):
    return pl.pallas_call(
        order_body,
        out_shape=jax.ShapeDtypeStruct((CAMS, 2 * own.shape[0] // CAMS * LANES), F32),
        in_specs=[SMEM, VMEM, VMEM],
        out_specs=VMEM,
        name="order",
    )(core, own, other)


def exchanged(pieces, axes):
    return lax.all_to_all(pieces, axes, 0, 0, tiled=True)


def from_all(share, axes):
    count = lax.axis_size(axes)
    return exchanged(jnp.broadcast_to(share[None], (count, *share.shape)), axes)


def to_owner(share):
    pairs = []
    for level in range(8):
        for column in range(4):
            pairs.append((level * 4 + column, (2 * column + level // 4) * 4 + level % 4))
    return lax.ppermute(share, ("z", "x"), pairs)


def turned(share, turn):
    count = lax.axis_size("x")
    return lax.ppermute(share, "x", [(k, (k + turn) % count) for k in range(count)])


def local(jacobians, residuals, camera_local, bucket_counts, camera_map):
    targets = lax.axis_size(PLANE)
    levels = lax.axis_size("z")
    level, core = lax.axis_index("z"), lax.axis_index("c")
    hot = jnp.argmax(bucket_counts[0])
    ids = camera_map.reshape(4, 2, 4, 2, QUARTERS, SPAN)
    ids = lax.dynamic_slice(ids, (0, level // 4, 0, 0, level % 4, 0), (4, 1, 4, 2, 1, SPAN))
    ids = ids.reshape(4, 4, 2, SPAN).transpose(1, 2, 0, 3).reshape(targets, 2, LANES)
    hot_ids = lax.dynamic_slice_in_dim(camera_map, hot * CAM_DEV, CAM_DEV)
    hot_ids = jnp.where(level == 0, hot_ids, -1).reshape(-1, 2, LANES)
    ids = jnp.concatenate([ids, hot_ids], axis=0)

    cameras = camera_local.reshape(1, -1)
    sent = packed(jacobians, residuals, cameras, bucket_counts, targets)
    arrived = exchanged(sent, PLANE)
    share = exchanged(camera_sums(arrived.reshape(-1, LANES)), "z").sum(axis=0)
    squares = to_owner(share[GRAD_ROWS:])
    slots = from_all(share[:GRAD_ROWS], PLANE)
    slots, squares = lax.optimization_barrier((slots, squares))
    shares = [squares] + [turned(squares, turn) for turn in range(1, QUARTERS)]
    first = lax.axis_index(PLANE) * levels * SPAN
    part = placed(slots, ids, first.reshape(1, 1), levels)
    part = exchanged(part, "z").sum(axis=0)
    part, shares = lax.optimization_barrier((part, shares))
    part = from_all(part, "z")
    own = (hot == lax.axis_index(OBS)).astype(jnp.int32)
    blocks = whole_blocks(jnp.stack([lax.axis_index("x"), own]).reshape(1, 2), shares, slots)
    part = from_all(part.reshape(-1, LANES), ("y", "x")).reshape(-1, LANES)
    other = lax.ppermute(part, "c", [(0, 1), (1, 0)])
    gradient = ordered(core.reshape(1, 1), part, other)
    return gradient, blocks


def solution(mesh):
    split = Mesh(mesh.devices.reshape(8, 4, 2, mesh.shape["rep"]), ALL)
    return jax.shard_map(
        local,
        mesh=split,
        in_specs=(P(None, ALL), P(None, ALL), P(ALL), P(ALL, None), P()),
        out_specs=(P(), P(None, OBS)),
        check_vma=False,
    )
```

```python
import jax
import jax.numpy as jnp
from jax import lax
from jax.experimental import pallas as pl
from jax.experimental.pallas import tpu as pltpu
from jax.sharding import Mesh
from jax.sharding import PartitionSpec as P

CAM_DEV = 1024
HALF = 256
LANES = 128
SPAN = 256
QUARTERS = CAM_DEV // SPAN
CAMS = 9
PAIRS = 45
TERMS = 56
VALUES = 21
BLOCK = 26
HOT_ROWS = 14
EXTRA_ROWS = 16
GRAD_ROWS = 2 * CAMS + HOT_ROWS
BLOCK_ROWS = 48
PAIRS_PER_STEP = 4
OBS = ("z", "y", "c")
PLANE = ("y", "c", "x")
ALL = ("z", "y", "c", "x")
F32 = jnp.float32
BF16 = jnp.bfloat16
VMEM = pl.BlockSpec(memory_space=pltpu.VMEM)
SMEM = pl.BlockSpec(memory_space=pltpu.SMEM)


def near(x):
    return pltpu.with_memory_space_constraint(x, pltpu.VMEM)


def two_pieces(x):
    upper = x.astype(BF16).astype(F32)
    return jnp.concatenate([upper, x - upper], axis=0).astype(BF16)


def kept_where(x, row, value):
    rows, lanes = x.shape
    kept = jnp.broadcast_to(row, (16, lanes)) == value
    kept = jnp.where(kept, 1.0, 0.0).astype(BF16)
    return (x.reshape(rows // 16, 16, lanes) * kept[None]).reshape(rows, lanes)


def one_hot(row):
    lanes = row.shape[1]
    spread = lax.broadcasted_iota(jnp.int32, (SPAN, lanes), 0) == row
    return jnp.where(spread, 1.0, 0.0).astype(BF16)


def product(left, right):
    return lax.dot_general(left, right, (((1,), (1,)), ((), ())), preferred_element_type=F32)


def set_operands(left_ref, right_ref, x, ids, parts, at):
    pieces = two_pieces(x)
    rows = pieces.shape[0]
    upper, lower = jnp.right_shift(ids, 8), jnp.bitwise_and(ids, SPAN - 1)
    for part in range(parts):
        left_ref[part * rows : (part + 1) * rows, at : at + LANES] = kept_where(pieces, upper, part)
    right_ref[:, at : at + LANES] = one_hot(lower)


def hot_piece(block):
    return slice(4 * block, min(4 * block + 4, HOT_ROWS))


def pack_body(counts_ref, jac_ref, res_ref, cam_ref, out_ref, terms_ref, left_ref, right_ref):
    targets = out_ref.shape[0]
    capacity = jac_ref.shape[1] // (2 * targets)

    def send(target, hot):
        for side in range(2):
            bucket = (2 * lax.rem(target, 4) + side) * 8 + lax.div(target, 4)
            count = counts_ref[0, bucket]
            for half in range(2):
                at = pl.multiple_of(bucket * capacity + half * LANES, LANES)
                here = pl.ds(at, LANES)
                live = lax.broadcasted_iota(jnp.int32, (1, LANES), 1) + half * LANES < count
                row = (2 * side + half) * BLOCK
                out_ref[target, row : row + 18, :] = jnp.where(live, jac_ref[:, here], 0.0)
                out_ref[target, row + 18 : row + 20, :] = jnp.where(live, res_ref[:, here], 0.0)
                out_ref[target, row + 20 : row + 21, :] = cam_ref[:, here].astype(F32)
            hot = jnp.where(count > HALF, bucket, hot)
        return hot

    hot = lax.fori_loop(0, targets, send, 0)
    for half in range(2):
        at = pl.multiple_of(hot * capacity + HALF + half * LANES, LANES)
        here = pl.ds(at, LANES)
        count = counts_ref[0, hot]
        live = lax.broadcasted_iota(jnp.int32, (1, LANES), 1) + HALF + half * LANES < count
        jac = jnp.where(live, jac_ref[:, here], 0.0)
        res = jnp.where(live, res_ref[:, here], 0.0)
        ids = cam_ref[:, here]
        first, second = jac[:CAMS], jac[CAMS:]
        for turn in range(5):
            around = first if turn == 0 else jnp.concatenate([first[turn:], first[:turn]], axis=0)
            beside = second if turn == 0 else jnp.concatenate([second[turn:], second[:turn]], axis=0)
            terms_ref[CAMS * turn : CAMS * (turn + 1), :] = first * around + second * beside
        terms_ref[PAIRS : PAIRS + CAMS, :] = first * res[0:1] + second * res[1:2]
        terms_ref[PAIRS + CAMS : TERMS, :] = jnp.zeros((TERMS - PAIRS - CAMS, LANES), F32)
        set_operands(left_ref, right_ref, terms_ref[...], ids, QUARTERS, half * LANES)
    summed = product(left_ref[...], right_ref[...])
    for share in range(targets):
        rows, column = HOT_ROWS * (share // 8), LANES * (share % 8)
        start = 2 * TERMS * (column // SPAN) + rows
        lanes = slice(column % SPAN, column % SPAN + LANES)
        piece = (
            summed[start : start + HOT_ROWS, lanes]
            + summed[start + TERMS : start + TERMS + HOT_ROWS, lanes]
        )
        for block in range(4):
            part = piece[hot_piece(block)]
            row = block * BLOCK + VALUES
            out_ref[share, row : row + part.shape[0], :] = part


def packed(jacobians, residuals, cameras, counts, targets):
    return pl.pallas_call(
        pack_body,
        out_shape=jax.ShapeDtypeStruct((targets, 4 * BLOCK, LANES), F32),
        in_specs=[SMEM, VMEM, VMEM, VMEM],
        out_specs=VMEM,
        scratch_shapes=[
            pltpu.VMEM((TERMS, LANES), F32),
            pltpu.VMEM((2 * TERMS * QUARTERS, 2 * LANES), BF16),
            pltpu.VMEM((SPAN, 2 * LANES), BF16),
        ],
        name="pack",
    )(counts, jacobians, residuals, cameras)


def sums_body(arrived_ref, out_ref, terms_ref, left_ref, right_ref, acc_ref, hot_ref):
    step = pl.program_id(0)

    @pl.when(step == 0)
    def _():
        acc_ref[...] = jnp.zeros_like(acc_ref)
        terms_ref[...] = jnp.zeros_like(terms_ref)
        hot_ref[...] = jnp.zeros_like(hot_ref)

    for pair in range(PAIRS_PER_STEP):
        start = pair * 8 * BLOCK
        value = [arrived_ref[pl.ds(start + row, 8, stride=BLOCK), :] for row in range(VALUES)]
        for turn in range(5):
            for k in range(CAMS):
                other = (k + turn) % CAMS
                term = value[k] * value[other] + value[CAMS + k] * value[CAMS + other]
                terms_ref[pair, pl.ds(CAMS * turn + k, 8, stride=TERMS), :] = term
        for k in range(CAMS):
            term = value[k] * value[18] + value[CAMS + k] * value[19]
            terms_ref[pair, pl.ds(PAIRS + k, 8, stride=TERMS), :] = term
        ids = value[20].astype(jnp.int32)
        for group in range(8):
            x = terms_ref[pair, group * TERMS : (group + 1) * TERMS, :]
            side = group % 4 // 2
            at = (group // 4 * 2 + group % 2) * LANES
            row = ids[group : group + 1, :]
            set_operands(left_ref.at[pair, side], right_ref.at[pair, side], x, row, QUARTERS, at)
        for source in range(2):
            for block in range(4):
                part = hot_piece(block)
                row = start + (source * 4 + block) * BLOCK + VALUES
                hot_ref[part, :] += arrived_ref[row : row + part.stop - part.start, :]
        for side in range(2):
            acc_ref[side] += product(left_ref[pair, side], right_ref[pair, side])

    @pl.when(step == pl.num_programs(0) - 1)
    def _():
        for side in range(2):
            for part in range(QUARTERS):
                at = 2 * TERMS * part
                both = acc_ref[side, at : at + TERMS, :] + acc_ref[side, at + TERMS : at + 2 * TERMS, :]
                level = side * QUARTERS + part
                for half in range(2):
                    lanes = slice(half * LANES, (half + 1) * LANES)
                    at = GRAD_ROWS + half * BLOCK_ROWS
                    out_ref[level, at : at + BLOCK_ROWS, :] = both[:BLOCK_ROWS, lanes]
                    out_ref[level, half * CAMS : (half + 1) * CAMS, :] = both[PAIRS : PAIRS + CAMS, lanes]
                out_ref[level, 2 * CAMS : GRAD_ROWS, :] = hot_ref[:HOT_ROWS]


def camera_sums(arrived):
    rows = arrived.shape[0]
    depth = 4 * LANES
    step = 8 * BLOCK * PAIRS_PER_STEP
    out = (2 * QUARTERS, GRAD_ROWS + 2 * BLOCK_ROWS, LANES)
    return pl.pallas_call(
        sums_body,
        grid=(rows // step,),
        out_shape=jax.ShapeDtypeStruct(out, F32),
        in_specs=[pl.BlockSpec((step, LANES), lambda i: (i, 0))],
        out_specs=pl.BlockSpec(out, lambda i: (0, 0, 0)),
        scratch_shapes=[
            pltpu.VMEM((PAIRS_PER_STEP, 8 * TERMS, LANES), F32),
            pltpu.VMEM((PAIRS_PER_STEP, 2, 2 * TERMS * QUARTERS, depth), BF16),
            pltpu.VMEM((PAIRS_PER_STEP, 2, SPAN, depth), BF16),
            pltpu.VMEM((2, 2 * TERMS * QUARTERS, SPAN), F32),
            pltpu.VMEM((EXTRA_ROWS, LANES), F32),
        ],
        cost_estimate=pl.CostEstimate(
            flops=2 * 2 * TERMS * CAM_DEV * 128 * rows // BLOCK, transcendentals=0, bytes_accessed=rows * 512
        ),
        name="sums",
    )(arrived)


def place_body(slots_ref, codes_ref, out_ref, left_ref, right_ref, acc_ref):
    sources = slots_ref.shape[0]
    ranges = out_ref.shape[0]
    blank = jnp.zeros((16 - CAMS, LANES), F32)

    def set_group(x, codes, chunk, group):
        x = jnp.concatenate([x, blank], axis=0)
        set_operands(left_ref.at[chunk], right_ref.at[chunk], x, codes, ranges, group * LANES)

    for chunk in range(sources // 4):
        for group in range(8):
            source, half = chunk * 4 + group // 2, group % 2
            x = slots_ref[source, half * CAMS : (half + 1) * CAMS, :]
            set_group(x, codes_ref[source, half : half + 1, :], chunk, group)
        summed = product(left_ref[chunk], right_ref[chunk])
        acc_ref[...] = summed if chunk == 0 else acc_ref[...] + summed
    row = 2 * CAMS + PAIRS % HOT_ROWS
    for group in range(4):
        x = slots_ref[PAIRS // HOT_ROWS * 4 + group, row : row + CAMS, :]
        set_group(x, codes_ref[sources + group // 2, group % 2 : group % 2 + 1, :], sources // 4, group)
    depth = 4 * LANES
    acc_ref[...] += product(left_ref[sources // 4, :, :depth], right_ref[sources // 4, :, :depth])
    for part in range(ranges):
        at = 32 * part
        both = acc_ref[at : at + CAMS, :] + acc_ref[at + 16 : at + 16 + CAMS, :]
        out_ref[part, :CAMS, :] = both[:, :LANES]
        out_ref[part, CAMS:, :] = both[:, LANES:]


def placed(slots, codes, ranges):
    depth = 8 * LANES
    chunks = slots.shape[0] // 4 + 1
    return pl.pallas_call(
        place_body,
        out_shape=jax.ShapeDtypeStruct((ranges, 2 * CAMS, LANES), F32),
        in_specs=[VMEM, VMEM],
        out_specs=VMEM,
        scratch_shapes=[
            pltpu.VMEM((chunks, 32 * ranges, depth), BF16),
            pltpu.VMEM((chunks, SPAN, depth), BF16),
            pltpu.VMEM((32 * ranges, SPAN), F32),
        ],
        name="place",
    )(near(slots), near(codes))


def blocks_body(place_ref, one_ref, two_ref, three_ref, four_ref, hot_ref, other_ref, out_ref, rows_ref):
    column, core, own = place_ref[0, 0], place_ref[0, 1], place_ref[0, 2]
    for turn, share_ref in enumerate((one_ref, two_ref, three_ref, four_ref)):
        part = lax.rem(column - turn + QUARTERS, QUARTERS)
        for half in range(2):
            for group in range(4):
                start, stop = HOT_ROWS * group, min(HOT_ROWS * (group + 1), PAIRS)
                source = group * 4 + lax.rem(part, 2) * 2 + half
                here = hot_ref[source, : stop - start, :]
                there = other_ref[source, : stop - start, :]
                hot = jnp.where(lax.div(part, 2) == core, here, there)
                share = share_ref[half * BLOCK_ROWS + start : half * BLOCK_ROWS + stop, :]
                rows_ref[start:stop, :] = share + jnp.where(own > 0, hot, 0.0)
            lanes = pl.ds(pl.multiple_of((part * 2 + half) * LANES, LANES), LANES)
            for k in range(CAMS):
                for l in range(CAMS):
                    ahead, behind = (l - k) % CAMS, (k - l) % CAMS
                    row = CAMS * ahead + k if ahead <= 4 else CAMS * behind + l
                    at = k * CAMS + l
                    out_ref[at : at + 1, lanes] = rows_ref[row : row + 1, :]


def whole_blocks(place, shares, hot, other):
    return pl.pallas_call(
        blocks_body,
        out_shape=jax.ShapeDtypeStruct((CAMS * CAMS, CAM_DEV), F32),
        in_specs=[SMEM] + [VMEM] * 6,
        out_specs=VMEM,
        scratch_shapes=[pltpu.VMEM((BLOCK_ROWS, LANES), F32)],
        name="blocks",
    )(place, *[near(x) for x in (*shares, hot, other)])


def order_body(core_ref, rows_ref, *refs):
    out_ref = refs[-1]
    tiles = rows_ref.shape[1] // CAMS
    ends = out_ref.shape[1] // (tiles * LANES)
    for end in range(ends):
        source = pl.program_id(0) * ends + end
        for tile in range(tiles):
            at = (end * tiles + tile) * LANES
            out_ref[:, at : at + LANES] = rows_ref[source, tile * CAMS : (tile + 1) * CAMS, :]


def ordered(core, rows, before=None):
    ends, depth, lanes = rows.shape
    steps = 4
    width = ends // steps * depth // CAMS * lanes
    whole = jax.ShapeDtypeStruct((CAMS, 2 * steps * width), F32)
    in_specs = [VMEM]
    operands, aliases = [core, near(rows)], {}
    if before is not None:
        in_specs.append(pl.BlockSpec(memory_space=pl.ANY))
        operands.append(before)
        aliases = {2: 0}
    return pl.pallas_call(
        order_body,
        grid_spec=pltpu.PrefetchScalarGridSpec(
            num_scalar_prefetch=1,
            grid=(steps,),
            in_specs=in_specs,
            out_specs=pl.BlockSpec((CAMS, width), lambda i, core: (0, core[0] * steps + i)),
        ),
        out_shape=whole,
        input_output_aliases=aliases,
        name="order",
    )(*operands)


def exchanged(pieces, axes):
    return lax.all_to_all(pieces, axes, 0, 0, tiled=True)


def from_all(share, axes):
    count = lax.axis_size(axes)
    return exchanged(jnp.broadcast_to(share[None], (count, *share.shape)), axes)


def to_owner(share):
    pairs = []
    for level in range(8):
        for column in range(4):
            pairs.append((level * 4 + column, (2 * column + level // 4) * 4 + level % 4))
    return lax.ppermute(share, ("z", "x"), pairs)


def turned(share, turn):
    count = lax.axis_size("x")
    return lax.ppermute(share, "x", [(k, (k + turn) % count) for k in range(count)])


def swapped(mine):
    return lax.ppermute(mine, "c", [(0, 1), (1, 0)])


def local(jacobians, residuals, camera_local, bucket_counts, camera_map):
    targets = lax.axis_size(PLANE)
    level, core = lax.axis_index("z"), lax.axis_index("c")
    hot = jnp.argmax(bucket_counts[0])
    ids = camera_map.reshape(4, 2, 4, 2, QUARTERS, SPAN)
    ids = lax.dynamic_slice(ids, (0, level // 4, 0, core, level % 4, 0), (4, 1, 4, 1, 1, SPAN))
    ids = ids.reshape(4, 4, SPAN).transpose(1, 0, 2).reshape(-1, 2, LANES)
    hot_ids = lax.dynamic_slice_in_dim(camera_map, hot * CAM_DEV + core * 4 * LANES, 4 * LANES)
    hot_ids = jnp.where(level == 0, hot_ids, -1).reshape(-1, 2, LANES)
    ids = jnp.concatenate([ids, hot_ids], axis=0)
    here = jnp.bitwise_and(jnp.right_shift(ids, 11), 15) == lax.axis_index(("y", "x"))
    codes = jnp.right_shift(ids, 15) * 8 * SPAN + jnp.bitwise_and(ids, 8 * SPAN - 1)
    codes = jnp.where(here & (ids >= 0), codes, -SPAN)

    cameras = camera_local.reshape(1, -1)
    sent = packed(jacobians, residuals, cameras, bucket_counts, targets)
    arrived = exchanged(sent, PLANE)
    share = exchanged(camera_sums(arrived.reshape(-1, LANES)), "z").sum(axis=0)
    squares = to_owner(share[GRAD_ROWS:])
    slots = from_all(share[:GRAD_ROWS], ("y", "x"))
    slots, squares = lax.optimization_barrier((slots, squares))
    shares = [squares] + [turned(squares, turn) for turn in range(1, QUARTERS)]
    part = placed(slots, codes, 16)
    own_hot = slots[:, 2 * CAMS :]
    other_hot = swapped(own_hot)
    part = exchanged(part, ("c", "z")).sum(axis=0)
    part, shares, other_hot = lax.optimization_barrier((part, shares, other_hot))
    part = from_all(part, "z")
    own = (hot == lax.axis_index(OBS)).astype(jnp.int32)
    place = jnp.stack([lax.axis_index("x"), core, own]).reshape(1, 3)
    blocks = whole_blocks(place, shares, own_hot, other_hot)
    part = from_all(part.reshape(-1, LANES), ("y", "x"))
    part, blocks = lax.optimization_barrier((part, blocks))
    other = swapped(part)
    gradient = ordered(core.reshape(1), part)
    gradient = ordered((1 - core).reshape(1), other, gradient)
    return gradient, blocks


def solution(mesh):
    split = Mesh(mesh.devices.reshape(8, 4, 2, mesh.shape["rep"]), ALL)
    return jax.shard_map(
        local,
        mesh=split,
        in_specs=(P(None, ALL), P(None, ALL), P(ALL), P(ALL, None), P()),
        out_specs=(P(), P(None, OBS)),
        check_vma=False,
    )
```

```python
import jax
import jax.numpy as jnp
from jax import lax
from jax.experimental import pallas as pl
from jax.experimental.pallas import tpu as pltpu
from jax.sharding import Mesh
from jax.sharding import PartitionSpec as P

CAM_DEV = 1024
HALF = 256
LANES = 128
SPAN = 256
QUARTERS = CAM_DEV // SPAN
CAMS = 9
PAIRS = 45
TERMS = 56
VALUES = 21
BLOCK = 28
HOT_ROWS = 7
GRAD_ROWS = 32
BLOCK_ROWS = 48
CHUNKS_PER_STEP = 4
OBS = ("zk", "zp", "y", "c")
ALL = ("zk", "zp", "y", "c", "x")
NEAR = ("zp", "y", "c", "x")
RANGE = ("zp", "y", "x")
F32 = jnp.float32
BF16 = jnp.bfloat16
VMEM = pl.BlockSpec(memory_space=pltpu.VMEM)
SMEM = pl.BlockSpec(memory_space=pltpu.SMEM)


def near(x):
    return pltpu.with_memory_space_constraint(x, pltpu.VMEM)


def two_pieces(x):
    upper = x.astype(BF16).astype(F32)
    return jnp.concatenate([upper, x - upper], axis=0).astype(BF16)


def kept_where(x, row, value):
    rows, lanes = x.shape
    kept = jnp.broadcast_to(row, (16, lanes)) == value
    kept = jnp.where(kept, 1.0, 0.0).astype(BF16)
    return (x.reshape(rows // 16, 16, lanes) * kept[None]).reshape(rows, lanes)


def one_hot(row):
    lanes = row.shape[1]
    spread = lax.broadcasted_iota(jnp.int32, (SPAN, lanes), 0) == row
    return jnp.where(spread, 1.0, 0.0).astype(BF16)


def product(left, right):
    return lax.dot_general(left, right, (((1,), (1,)), ((), ())), preferred_element_type=F32)


def set_operands(left_ref, right_ref, x, ids, parts, at):
    pieces = two_pieces(x)
    rows = pieces.shape[0]
    upper, lower = jnp.right_shift(ids, 8), jnp.bitwise_and(ids, SPAN - 1)
    for part in range(parts):
        left_ref[part * rows : (part + 1) * rows, at : at + LANES] = kept_where(pieces, upper, part)
    right_ref[:, at : at + LANES] = one_hot(lower)


def pack_body(
    counts_ref, jac_ref, res_ref, cam_ref, out_ref, kept_ref, terms_ref, left_ref, right_ref
):
    targets = out_ref.shape[0]
    capacity = jac_ref.shape[1] // 16
    step = pl.program_id(0)
    hot = jnp.int32(-1)
    for side in range(2):
        for owner in range(8):
            bucket = side * 8 + owner
            count = counts_ref[0, step * 16 + bucket]
            target = side * 32 + owner * 4 + step
            for half in range(2):
                at = bucket * capacity + half * LANES
                here = slice(at, at + LANES)
                live = lax.broadcasted_iota(jnp.int32, (1, LANES), 1) + half * LANES < count
                row = half * BLOCK
                out_ref[target, row : row + 18, :] = jnp.where(live, jac_ref[:, here], 0.0)
                out_ref[target, row + 18 : row + 20, :] = jnp.where(live, res_ref[:, here], 0.0)
                out_ref[target, row + 20 : row + 21, :] = cam_ref[:, here].astype(F32)
            hot = jnp.where(count > HALF, bucket, hot)

    @pl.when(hot >= 0)
    def _():
        count = counts_ref[0, step * 16 + hot]
        for half in range(2):
            at = pl.multiple_of(hot * capacity + HALF + half * LANES, LANES)
            here = pl.ds(at, LANES)
            live = lax.broadcasted_iota(jnp.int32, (1, LANES), 1) + HALF + half * LANES < count
            kept_ref[half, :18, :] = jnp.where(live, jac_ref[:, here], 0.0)
            kept_ref[half, 18:20, :] = jnp.where(live, res_ref[:, here], 0.0)
            kept_ref[half, 20:21, :] = cam_ref[:, here].astype(F32)

    @pl.when(step == pl.num_programs(0) - 1)
    def _():
        for half in range(2):
            kept = kept_ref[half]
            first, second = kept[:CAMS], kept[CAMS : 2 * CAMS]
            for turn in range(5):
                around = first if turn == 0 else jnp.concatenate([first[turn:], first[:turn]], axis=0)
                beside = second if turn == 0 else jnp.concatenate([second[turn:], second[:turn]], axis=0)
                terms_ref[CAMS * turn : CAMS * (turn + 1), :] = first * around + second * beside
            terms_ref[PAIRS : PAIRS + CAMS, :] = first * kept[18:19] + second * kept[19:20]
            terms_ref[PAIRS + CAMS : TERMS, :] = jnp.zeros((TERMS - PAIRS - CAMS, LANES), F32)
            ids = kept[20:21].astype(jnp.int32)
            set_operands(left_ref, right_ref, terms_ref[...], ids, QUARTERS, half * LANES)
        summed = product(left_ref[...], right_ref[...])
        for share in range(targets):
            rows, column = HOT_ROWS * (share // 8), LANES * (share % 8)
            start = 2 * TERMS * (column // SPAN) + rows
            lanes = slice(column % SPAN, column % SPAN + LANES)
            piece = (
                summed[start : start + HOT_ROWS, lanes]
                + summed[start + TERMS : start + TERMS + HOT_ROWS, lanes]
            )
            out_ref[share, VALUES : VALUES + HOT_ROWS, :] = piece


def packed(jacobians, residuals, cameras, counts, targets):
    steps = 4
    width = jacobians.shape[1] // steps
    return pl.pallas_call(
        pack_body,
        grid=(steps,),
        out_shape=pltpu.VMEM((targets, 2 * BLOCK, LANES), F32),
        in_specs=[
            SMEM,
            pl.BlockSpec((18, width), lambda i: (0, i)),
            pl.BlockSpec((2, width), lambda i: (0, i)),
            pl.BlockSpec((1, width), lambda i: (0, i)),
        ],
        out_specs=VMEM,
        scratch_shapes=[
            pltpu.VMEM((2, 24, LANES), F32),
            pltpu.VMEM((TERMS, LANES), F32),
            pltpu.VMEM((2 * TERMS * QUARTERS, 2 * LANES), BF16),
            pltpu.VMEM((SPAN, 2 * LANES), BF16),
        ],
        name="pack",
    )(counts, jacobians, residuals, cameras)


def sums_body(arrived_ref, *refs):
    out_refs, (terms_ref, left_ref, right_ref, acc_ref, hot_ref) = refs[:QUARTERS], refs[QUARTERS:]
    step = pl.program_id(0)

    @pl.when(step == 0)
    def _():
        acc_ref[...] = jnp.zeros_like(acc_ref)
        terms_ref[...] = jnp.zeros_like(terms_ref)
        hot_ref[...] = jnp.zeros_like(hot_ref)

    for chunk in range(CHUNKS_PER_STEP):
        start = chunk * 8 * BLOCK
        value = [arrived_ref[pl.ds(start + row, 8, stride=BLOCK), :] for row in range(VALUES)]
        for turn in range(5):
            for k in range(CAMS):
                other = (k + turn) % CAMS
                term = value[k] * value[other] + value[CAMS + k] * value[CAMS + other]
                terms_ref[chunk, pl.ds(CAMS * turn + k, 8, stride=TERMS), :] = term
        for k in range(CAMS):
            term = value[k] * value[18] + value[CAMS + k] * value[19]
            terms_ref[chunk, pl.ds(PAIRS + k, 8, stride=TERMS), :] = term
        ids = value[20].astype(jnp.int32)
        for group in range(8):
            x = terms_ref[chunk, group * TERMS : (group + 1) * TERMS, :]
            row = ids[group : group + 1, :]
            set_operands(left_ref.at[chunk], right_ref.at[chunk], x, row, QUARTERS, group * LANES)
        for source in range(4):
            row = start + 2 * source * BLOCK + VALUES
            hot_ref[:HOT_ROWS, :] += arrived_ref[row : row + HOT_ROWS, :]
        acc_ref[...] += product(left_ref[chunk], right_ref[chunk])

    @pl.when(step == pl.num_programs(0) - 1)
    def _():
        for turn, out_ref in enumerate(out_refs):
            part = lax.rem(lax.axis_index("zk") + turn, QUARTERS)
            upper = pl.ds(pl.multiple_of(2 * TERMS * part, 16), TERMS)
            lower = pl.ds(pl.multiple_of(2 * TERMS * part + TERMS, 8), TERMS)
            both = acc_ref[upper, :] + acc_ref[lower, :]
            for half in range(2):
                lanes = slice(half * LANES, (half + 1) * LANES)
                at = GRAD_ROWS + half * BLOCK_ROWS
                out_ref[at : at + BLOCK_ROWS, :] = both[:BLOCK_ROWS, lanes]
                out_ref[half * CAMS : (half + 1) * CAMS, :] = both[PAIRS : PAIRS + CAMS, lanes]
            out_ref[2 * CAMS : 2 * CAMS + HOT_ROWS, :] = hot_ref[:HOT_ROWS]
            rest = GRAD_ROWS - 2 * CAMS - HOT_ROWS
            out_ref[GRAD_ROWS - rest : GRAD_ROWS, :] = jnp.zeros((rest, LANES), F32)


def camera_sums(arrived):
    rows = arrived.shape[0]
    depth = 8 * LANES
    step = 8 * BLOCK * CHUNKS_PER_STEP
    out = (GRAD_ROWS + 2 * BLOCK_ROWS, LANES)
    return pl.pallas_call(
        sums_body,
        grid=(rows // step,),
        out_shape=[pltpu.VMEM(out, F32)] * QUARTERS,
        in_specs=[pl.BlockSpec((step, LANES), lambda i: (i, 0))],
        out_specs=[VMEM] * QUARTERS,
        scratch_shapes=[
            pltpu.VMEM((CHUNKS_PER_STEP, 8 * TERMS, LANES), F32),
            pltpu.VMEM((CHUNKS_PER_STEP, 2 * TERMS * QUARTERS, depth), BF16),
            pltpu.VMEM((CHUNKS_PER_STEP, SPAN, depth), BF16),
            pltpu.VMEM((2 * TERMS * QUARTERS, SPAN), F32),
            pltpu.VMEM((8, LANES), F32),
        ],
        cost_estimate=pl.CostEstimate(
            flops=2 * 2 * TERMS * CAM_DEV * 128 * rows // BLOCK, transcendentals=0, bytes_accessed=rows * 512
        ),
        name="sums",
    )(arrived)


def place_body(slots_ref, codes_ref, mine_ref, theirs_ref, left_ref, right_ref, acc_ref):
    sources = slots_ref.shape[0]
    ranges = acc_ref.shape[0] // 32
    blank = jnp.zeros((16 - CAMS, LANES), F32)

    def set_group(x, codes, chunk, group):
        x = jnp.concatenate([x, blank], axis=0)
        set_operands(left_ref.at[chunk], right_ref.at[chunk], x, codes, ranges, group * LANES)

    for chunk in range(sources // 4):
        for group in range(8):
            source, half = chunk * 4 + group // 2, group % 2
            x = slots_ref[source, half * CAMS : (half + 1) * CAMS, :]
            set_group(x, codes_ref[source, half : half + 1, :], chunk, group)
        summed = product(left_ref[chunk], right_ref[chunk])
        acc_ref[...] = summed if chunk == 0 else acc_ref[...] + summed
    split = HOT_ROWS - PAIRS % HOT_ROWS
    for group in range(4):
        source = PAIRS // HOT_ROWS * 4 + group
        x = slots_ref[source, 2 * CAMS + HOT_ROWS - split : 2 * CAMS + HOT_ROWS, :]
        rest = slots_ref[source + 4, 2 * CAMS : 3 * CAMS - split, :]
        x = jnp.concatenate([x, rest], axis=0)
        set_group(x, codes_ref[sources + group // 2, group % 2 : group % 2 + 1, :], sources // 4, group)
    depth = 4 * LANES
    acc_ref[...] += product(left_ref[sources // 4, :, :depth], right_ref[sources // 4, :, :depth])
    for flip, out_ref in enumerate((mine_ref, theirs_ref)):
        core = jnp.bitwise_xor(lax.axis_index("c"), flip)
        for part in range(QUARTERS):
            at = pl.multiple_of((core * QUARTERS + part) * 32, 32)
            both = acc_ref[pl.ds(at, CAMS), :] + acc_ref[pl.ds(at + 16, CAMS), :]
            for half in range(2):
                row = (part * 2 + half) * CAMS
                out_ref[row : row + CAMS, :] = both[:, half * LANES : (half + 1) * LANES]


def placed(slots, codes, ranges):
    depth = 8 * LANES
    chunks = slots.shape[0] // 4 + 1
    return pl.pallas_call(
        place_body,
        out_shape=[pltpu.VMEM((ranges * CAMS, LANES), F32)] * 2,
        in_specs=[VMEM, VMEM],
        out_specs=[VMEM, VMEM],
        scratch_shapes=[
            pltpu.VMEM((chunks, 32 * ranges, depth), BF16),
            pltpu.VMEM((chunks, SPAN, depth), BF16),
            pltpu.VMEM((32 * ranges, SPAN), F32),
        ],
        name="place",
    )(near(slots), near(codes))


def blocks_body(counts_ref, one_ref, two_ref, three_ref, four_ref, hot_ref, other_ref, out_ref, rows_ref):
    column, core = lax.axis_index("x"), lax.axis_index("c")
    own = jnp.where(counts_ref[0, lax.axis_index(OBS)] > HALF, 1, 0)
    for turn, share_ref in enumerate((one_ref, two_ref, three_ref, four_ref)):
        part = lax.rem(column - turn + QUARTERS, QUARTERS)
        for half in range(2):
            for group in range(TERMS // HOT_ROWS):
                start, stop = HOT_ROWS * group, min(HOT_ROWS * (group + 1), PAIRS)
                if start >= PAIRS:
                    continue
                source = group * 4 + lax.rem(part, 2) * 2 + half
                here = hot_ref[source, : stop - start, :]
                there = other_ref[source, : stop - start, :]
                hot = jnp.where(lax.div(part, 2) == core, here, there)
                share = share_ref[half * BLOCK_ROWS + start : half * BLOCK_ROWS + stop, :]
                rows_ref[start:stop, :] = share + jnp.where(own > 0, hot, 0.0)
            lanes = pl.ds(pl.multiple_of((part * 2 + half) * LANES, LANES), LANES)
            for k in range(CAMS):
                for l in range(CAMS):
                    ahead, behind = (l - k) % CAMS, (k - l) % CAMS
                    row = CAMS * ahead + k if ahead <= 4 else CAMS * behind + l
                    at = k * CAMS + l
                    out_ref[at : at + 1, lanes] = rows_ref[row : row + 1, :]


def whole_blocks(counts, shares, hot, other):
    return pl.pallas_call(
        blocks_body,
        out_shape=jax.ShapeDtypeStruct((CAMS * CAMS, CAM_DEV), F32),
        in_specs=[SMEM] + [VMEM] * 6,
        out_specs=VMEM,
        scratch_shapes=[pltpu.VMEM((BLOCK_ROWS, LANES), F32)],
        name="blocks",
    )(counts, *[near(x) for x in (*shares, hot, other)])


def order_body(core_ref, rows_ref, *refs):
    out_ref = refs[-1]
    width = SPAN * QUARTERS
    ends = out_ref.shape[1] // width
    for end in range(ends):
        source = pl.program_id(0) * ends + end
        for tile in range(width // LANES):
            at = end * width + tile * LANES
            out_ref[:, at : at + LANES] = rows_ref[source, tile * CAMS : (tile + 1) * CAMS, :]


def ordered(core, rows, before=None):
    ends, depth, lanes = rows.shape
    steps = 4
    width = ends // steps * depth // CAMS * lanes
    whole = jax.ShapeDtypeStruct((CAMS, 2 * steps * width), F32)
    in_specs = [VMEM]
    operands, aliases, flip = [core, near(rows)], {}, int(before is not None)
    if before is not None:
        in_specs.append(pl.BlockSpec(memory_space=pl.ANY))
        operands.append(before)
        aliases = {2: 0}
    return pl.pallas_call(
        order_body,
        grid_spec=pltpu.PrefetchScalarGridSpec(
            num_scalar_prefetch=1,
            grid=(steps,),
            in_specs=in_specs,
            out_specs=pl.BlockSpec((CAMS, width), lambda i, core: (0, jnp.bitwise_xor(core[0], flip) * steps + i)),
        ),
        out_shape=whole,
        input_output_aliases=aliases,
        name="order",
    )(*operands)


def exchanged(pieces, axes):
    return lax.all_to_all(pieces, axes, 0, 0, tiled=True)


def from_all(share, axes):
    count = lax.axis_size(axes)
    return exchanged(jnp.broadcast_to(share[None], (count, *share.shape)), axes)


def to_owner(share):
    pairs = [(level * 4 + column, column * 4 + level) for level in range(4) for column in range(4)]
    return lax.ppermute(share, ("zk", "x"), pairs)


def turned(share, axis, turn):
    count = lax.axis_size(axis)
    return lax.ppermute(share, axis, [(k, (k + turn) % count) for k in range(count)])


def local(jacobians, residuals, camera_local, bucket_counts, camera_map):
    targets = lax.axis_size(NEAR)
    level, core = lax.axis_index("zk"), lax.axis_index("c")
    cameras = camera_local.reshape(1, -1)
    sent = packed(jacobians, residuals, cameras, bucket_counts, targets)
    arrived = exchanged(sent, NEAR)
    camera_map, bucket_counts, arrived = lax.optimization_barrier((camera_map, bucket_counts, arrived))
    hot = jnp.argmax(bucket_counts[0])
    ids = camera_map.reshape(4, 2, 4, 2, QUARTERS, SPAN)
    ids = lax.dynamic_slice(ids, (0, 0, 0, core, level, 0), (4, 2, 4, 1, 1, SPAN))
    ids = ids.reshape(4, 8, SPAN).transpose(1, 0, 2).reshape(-1, 2, LANES)
    hot_ids = lax.dynamic_slice_in_dim(camera_map, hot * CAM_DEV + core * 4 * LANES, 4 * LANES)
    hot_ids = jnp.where(level == 0, hot_ids, -1).reshape(-1, 2, LANES)
    ids = jnp.concatenate([ids, hot_ids], axis=0)
    here = jnp.bitwise_and(jnp.right_shift(ids, 10), 31) == lax.axis_index(RANGE)
    codes = jnp.right_shift(ids, 15) * QUARTERS * SPAN + jnp.bitwise_and(ids, QUARTERS * SPAN - 1)
    codes = jnp.where(here & (ids >= 0), codes, -SPAN)
    sums = camera_sums(arrived.reshape(-1, LANES))
    share = sums[0]
    for turn in range(1, QUARTERS):
        share = share + turned(sums[turn], "zk", turn)
    squares = to_owner(share[GRAD_ROWS:])
    slots = from_all(share[:GRAD_ROWS], RANGE)
    slots, squares = lax.optimization_barrier((slots, squares))
    shares = [squares] + [turned(squares, "x", turn) for turn in range(1, QUARTERS)]
    mine, theirs = placed(slots, codes, 2 * QUARTERS)
    own_hot = slots[:, 2 * CAMS : 2 * CAMS + HOT_ROWS]
    other_hot = turned(own_hot, "c", 1)
    mine = mine + turned(theirs, "c", 1)
    part = mine
    for turn in range(1, QUARTERS):
        part = part + turned(mine, "zk", turn)
    part, shares, other_hot = lax.optimization_barrier((part, shares, other_hot))
    blocks = whole_blocks(bucket_counts, shares, own_hot, other_hot)
    part = from_all(part, RANGE)
    part, blocks = lax.optimization_barrier((part, blocks))
    other = turned(part, "c", 1)
    core = core.reshape(1)
    gradient = ordered(core, part)
    gradient = ordered(core, other, gradient)
    return gradient, blocks


def solution(mesh):
    split = Mesh(mesh.devices.reshape(4, 2, 4, 2, mesh.shape["rep"]), ALL)
    return jax.shard_map(
        local,
        mesh=split,
        in_specs=(P(None, ALL), P(None, ALL), P(ALL), P(ALL, None), P()),
        out_specs=(P(), P(None, OBS)),
        check_vma=False,
    )
```

```python
import jax
import jax.numpy as jnp
from jax import lax
from jax.experimental import pallas as pl
from jax.experimental.pallas import tpu as pltpu
from jax.sharding import Mesh
from jax.sharding import PartitionSpec as P

CAM_DEV = 1024
HALF = 256
LANES = 128
SPAN = 256
QUARTERS = CAM_DEV // SPAN
CAMS = 9
PAIRS = 45
TERMS = 56
VALUES = 21
BLOCK = 26
HOT_ROWS = 7
HOT_FIRST = 5
GRAD_ROWS = 32
BLOCK_ROWS = 48
CHUNKS_PER_STEP = 4
OBS = ("zk", "zp", "y", "c")
ALL = ("zk", "zp", "y", "c", "x")
NEAR = ("zp", "y", "c", "x")
RANGE = ("zp", "y", "x")
F32 = jnp.float32
BF16 = jnp.bfloat16
VMEM = pl.BlockSpec(memory_space=pltpu.VMEM)
SMEM = pl.BlockSpec(memory_space=pltpu.SMEM)


def near(x):
    return pltpu.with_memory_space_constraint(x, pltpu.VMEM)


def two_pieces(x):
    upper = x.astype(BF16).astype(F32)
    return jnp.concatenate([upper, x - upper], axis=0).astype(BF16)


def kept_where(x, row, value):
    rows, lanes = x.shape
    kept = jnp.broadcast_to(row, (16, lanes)) == value
    kept = jnp.where(kept, 1.0, 0.0).astype(BF16)
    return (x.reshape(rows // 16, 16, lanes) * kept[None]).reshape(rows, lanes)


def one_hot(row):
    lanes = row.shape[1]
    spread = lax.broadcasted_iota(jnp.int32, (SPAN, lanes), 0) == row
    return jnp.where(spread, 1.0, 0.0).astype(BF16)


def product(left, right):
    return lax.dot_general(left, right, (((1,), (1,)), ((), ())), preferred_element_type=F32)


def set_operands(left_ref, right_ref, x, ids, parts, at):
    pieces = two_pieces(x)
    rows = pieces.shape[0]
    upper, lower = jnp.right_shift(ids, 8), jnp.bitwise_and(ids, SPAN - 1)
    for part in range(parts):
        left_ref[part * rows : (part + 1) * rows, at : at + LANES] = kept_where(pieces, upper, part)
    right_ref[:, at : at + LANES] = one_hot(lower)


def pack_body(
    counts_ref, jac_ref, res_ref, cam_ref, out_ref, kept_ref, terms_ref, left_ref, right_ref
):
    targets = out_ref.shape[0] // (2 * BLOCK)
    capacity = jac_ref.shape[1] // 16
    step = pl.program_id(0)
    for level in range(4):

        @pl.when(step == level)
        def _():
            for side in range(2):
                for owner in range(8):
                    bucket = side * 8 + owner
                    count = counts_ref[0, level * 16 + bucket]
                    target = side * 32 + owner * 4 + level
                    for half in range(2):
                        at = bucket * capacity + half * LANES
                        here = slice(at, at + LANES)
                        live = lax.broadcasted_iota(jnp.int32, (1, LANES), 1) + half * LANES < count
                        row = (2 * target + half) * BLOCK
                        out_ref[row : row + 18, :] = jnp.where(live, jac_ref[:, here], 0.0)
                        out_ref[row + 18 : row + 20, :] = jnp.where(live, res_ref[:, here], 0.0)
                        out_ref[row + 20 : row + 21, :] = cam_ref[:, here].astype(F32)

    hot = jnp.int32(-1)
    for bucket in range(16):
        hot = jnp.where(counts_ref[0, step * 16 + bucket] > HALF, bucket, hot)

    @pl.when(hot >= 0)
    def _():
        count = counts_ref[0, step * 16 + hot]
        for half in range(2):
            at = pl.multiple_of(hot * capacity + HALF + half * LANES, LANES)
            here = pl.ds(at, LANES)
            live = lax.broadcasted_iota(jnp.int32, (1, LANES), 1) + HALF + half * LANES < count
            kept_ref[half, :18, :] = jnp.where(live, jac_ref[:, here], 0.0)
            kept_ref[half, 18:20, :] = jnp.where(live, res_ref[:, here], 0.0)
            kept_ref[half, 20:21, :] = cam_ref[:, here].astype(F32)

    @pl.when(step == pl.num_programs(0) - 1)
    def _():
        for half in range(2):
            kept = kept_ref[half]
            first, second = kept[:CAMS], kept[CAMS : 2 * CAMS]
            for turn in range(5):
                around = first if turn == 0 else jnp.concatenate([first[turn:], first[:turn]], axis=0)
                beside = second if turn == 0 else jnp.concatenate([second[turn:], second[:turn]], axis=0)
                terms_ref[CAMS * turn : CAMS * (turn + 1), :] = first * around + second * beside
            terms_ref[PAIRS : PAIRS + CAMS, :] = first * kept[18:19] + second * kept[19:20]
            terms_ref[PAIRS + CAMS : TERMS, :] = jnp.zeros((TERMS - PAIRS - CAMS, LANES), F32)
            ids = kept[20:21].astype(jnp.int32)
            set_operands(left_ref, right_ref, terms_ref[...], ids, QUARTERS, half * LANES)
        summed = product(left_ref[...], right_ref[...])
        for share in range(targets):
            rows, column = HOT_ROWS * (share // 8), LANES * (share % 8)
            start = 2 * TERMS * (column // SPAN) + rows
            lanes = slice(column % SPAN, column % SPAN + LANES)
            piece = (
                summed[start : start + HOT_ROWS, lanes]
                + summed[start + TERMS : start + TERMS + HOT_ROWS, lanes]
            )
            row = 2 * share * BLOCK + VALUES
            out_ref[row : row + HOT_FIRST, :] = piece[:HOT_FIRST]
            row += BLOCK
            out_ref[row : row + HOT_ROWS - HOT_FIRST, :] = piece[HOT_FIRST:]


def packed(jacobians, residuals, cameras, counts, targets):
    steps = 4
    width = jacobians.shape[1] // steps
    return pl.pallas_call(
        pack_body,
        grid=(steps,),
        out_shape=pltpu.VMEM((targets * 2 * BLOCK, LANES), F32),
        in_specs=[
            SMEM,
            pl.BlockSpec((18, width), lambda i: (0, i)),
            pl.BlockSpec((2, width), lambda i: (0, i)),
            pl.BlockSpec((1, width), lambda i: (0, i)),
        ],
        out_specs=VMEM,
        scratch_shapes=[
            pltpu.VMEM((2, 24, LANES), F32),
            pltpu.VMEM((TERMS, LANES), F32),
            pltpu.VMEM((2 * TERMS * QUARTERS, 2 * LANES), BF16),
            pltpu.VMEM((SPAN, 2 * LANES), BF16),
        ],
        name="pack",
    )(counts, jacobians, residuals, cameras)


def sums_body(arrived_ref, *refs):
    out_refs, (terms_ref, left_ref, right_ref, acc_ref, hot_ref) = refs[:QUARTERS], refs[QUARTERS:]
    step = pl.program_id(0)

    @pl.when(step == 0)
    def _():
        acc_ref[...] = jnp.zeros_like(acc_ref)
        terms_ref[...] = jnp.zeros_like(terms_ref)
        hot_ref[...] = jnp.zeros_like(hot_ref)

    for chunk in range(CHUNKS_PER_STEP):
        start = chunk * 8 * BLOCK
        value = [arrived_ref[pl.ds(start + row, 8, stride=BLOCK), :] for row in range(VALUES)]
        for turn in range(5):
            for k in range(CAMS):
                other = (k + turn) % CAMS
                term = value[k] * value[other] + value[CAMS + k] * value[CAMS + other]
                terms_ref[chunk, pl.ds(CAMS * turn + k, 8, stride=TERMS), :] = term
        for k in range(CAMS):
            term = value[k] * value[18] + value[CAMS + k] * value[19]
            terms_ref[chunk, pl.ds(PAIRS + k, 8, stride=TERMS), :] = term
        ids = value[20].astype(jnp.int32)
        for group in range(8):
            x = terms_ref[chunk, group * TERMS : (group + 1) * TERMS, :]
            row = ids[group : group + 1, :]
            set_operands(left_ref.at[chunk], right_ref.at[chunk], x, row, QUARTERS, group * LANES)
        for source in range(4):
            row = start + 2 * source * BLOCK + VALUES
            hot_ref[:HOT_FIRST, :] += arrived_ref[row : row + HOT_FIRST, :]
            row += BLOCK
            rest = HOT_ROWS - HOT_FIRST
            hot_ref[HOT_FIRST:HOT_ROWS, :] += arrived_ref[row : row + rest, :]
        acc_ref[...] += product(left_ref[chunk], right_ref[chunk])

    @pl.when(step == pl.num_programs(0) - 1)
    def _():
        for turn, out_ref in enumerate(out_refs):
            part = lax.rem(lax.axis_index("zk") + turn, QUARTERS)
            upper = pl.ds(pl.multiple_of(2 * TERMS * part, 16), TERMS)
            lower = pl.ds(pl.multiple_of(2 * TERMS * part + TERMS, 8), TERMS)
            both = acc_ref[upper, :] + acc_ref[lower, :]
            for half in range(2):
                lanes = slice(half * LANES, (half + 1) * LANES)
                at = GRAD_ROWS + half * BLOCK_ROWS
                out_ref[at : at + BLOCK_ROWS, :] = both[:BLOCK_ROWS, lanes]
                out_ref[half * CAMS : (half + 1) * CAMS, :] = both[PAIRS : PAIRS + CAMS, lanes]
            out_ref[2 * CAMS : 2 * CAMS + HOT_ROWS, :] = hot_ref[:HOT_ROWS]
            rest = GRAD_ROWS - 2 * CAMS - HOT_ROWS
            out_ref[GRAD_ROWS - rest : GRAD_ROWS, :] = jnp.zeros((rest, LANES), F32)


def camera_sums(arrived):
    rows = arrived.shape[0]
    depth = 8 * LANES
    step = 8 * BLOCK * CHUNKS_PER_STEP
    out = (GRAD_ROWS + 2 * BLOCK_ROWS, LANES)
    return pl.pallas_call(
        sums_body,
        grid=(rows // step,),
        out_shape=[pltpu.VMEM(out, F32)] * QUARTERS,
        in_specs=[pl.BlockSpec((step, LANES), lambda i: (i, 0))],
        out_specs=[VMEM] * QUARTERS,
        scratch_shapes=[
            pltpu.VMEM((CHUNKS_PER_STEP, 8 * TERMS, LANES), F32),
            pltpu.VMEM((CHUNKS_PER_STEP, 2 * TERMS * QUARTERS, depth), BF16),
            pltpu.VMEM((CHUNKS_PER_STEP, SPAN, depth), BF16),
            pltpu.VMEM((2 * TERMS * QUARTERS, SPAN), F32),
            pltpu.VMEM((8, LANES), F32),
        ],
        cost_estimate=pl.CostEstimate(
            flops=2 * 2 * TERMS * CAM_DEV * 128 * rows // BLOCK, transcendentals=0, bytes_accessed=rows * 512
        ),
        name="sums",
    )(arrived)


def place_body(slots_ref, codes_ref, mine_ref, theirs_ref, left_ref, right_ref, acc_ref):
    sources = slots_ref.shape[0]
    ranges = acc_ref.shape[0] // 32
    blank = jnp.zeros((16 - CAMS, LANES), F32)

    def set_group(x, codes, chunk, group):
        x = jnp.concatenate([x, blank], axis=0)
        set_operands(left_ref.at[chunk], right_ref.at[chunk], x, codes, ranges, group * LANES)

    for chunk in range(sources // 4):
        for group in range(8):
            source, half = chunk * 4 + group // 2, group % 2
            x = slots_ref[source, half * CAMS : (half + 1) * CAMS, :]
            set_group(x, codes_ref[source, half : half + 1, :], chunk, group)
        summed = product(left_ref[chunk], right_ref[chunk])
        acc_ref[...] = summed if chunk == 0 else acc_ref[...] + summed
    split = HOT_ROWS - PAIRS % HOT_ROWS
    for group in range(4):
        source = PAIRS // HOT_ROWS * 4 + group
        x = slots_ref[source, 2 * CAMS + HOT_ROWS - split : 2 * CAMS + HOT_ROWS, :]
        rest = slots_ref[source + 4, 2 * CAMS : 3 * CAMS - split, :]
        x = jnp.concatenate([x, rest], axis=0)
        set_group(x, codes_ref[sources + group // 2, group % 2 : group % 2 + 1, :], sources // 4, group)
    depth = 4 * LANES
    acc_ref[...] += product(left_ref[sources // 4, :, :depth], right_ref[sources // 4, :, :depth])
    for flip, out_ref in enumerate((mine_ref, theirs_ref)):
        core = jnp.bitwise_xor(lax.axis_index("c"), flip)
        for part in range(QUARTERS):
            at = pl.multiple_of((core * QUARTERS + part) * 32, 32)
            both = acc_ref[pl.ds(at, CAMS), :] + acc_ref[pl.ds(at + 16, CAMS), :]
            for half in range(2):
                row = (part * 2 + half) * CAMS
                out_ref[row : row + CAMS, :] = both[:, half * LANES : (half + 1) * LANES]


def placed(slots, codes, ranges):
    depth = 8 * LANES
    chunks = slots.shape[0] // 4 + 1
    return pl.pallas_call(
        place_body,
        out_shape=[pltpu.VMEM((ranges * CAMS, LANES), F32)] * 2,
        in_specs=[VMEM, VMEM],
        out_specs=[VMEM, VMEM],
        scratch_shapes=[
            pltpu.VMEM((chunks, 32 * ranges, depth), BF16),
            pltpu.VMEM((chunks, SPAN, depth), BF16),
            pltpu.VMEM((32 * ranges, SPAN), F32),
        ],
        name="place",
    )(near(slots), near(codes))


def blocks_body(counts_ref, one_ref, two_ref, three_ref, four_ref, hot_ref, other_ref, out_ref, rows_ref):
    column, core = lax.axis_index("x"), lax.axis_index("c")
    own = jnp.where(counts_ref[0, lax.axis_index(OBS)] > HALF, 1, 0)
    for turn, share_ref in enumerate((one_ref, two_ref, three_ref, four_ref)):
        part = lax.rem(column - turn + QUARTERS, QUARTERS)
        for half in range(2):
            for group in range(TERMS // HOT_ROWS):
                start, stop = HOT_ROWS * group, min(HOT_ROWS * (group + 1), PAIRS)
                if start >= PAIRS:
                    continue
                source = group * 4 + lax.rem(part, 2) * 2 + half
                here = hot_ref[source, : stop - start, :]
                there = other_ref[source, : stop - start, :]
                hot = jnp.where(lax.div(part, 2) == core, here, there)
                share = share_ref[half * BLOCK_ROWS + start : half * BLOCK_ROWS + stop, :]
                rows_ref[start:stop, :] = share + jnp.where(own > 0, hot, 0.0)
            lanes = pl.ds(pl.multiple_of((part * 2 + half) * LANES, LANES), LANES)
            for k in range(CAMS):
                for l in range(CAMS):
                    ahead, behind = (l - k) % CAMS, (k - l) % CAMS
                    row = CAMS * ahead + k if ahead <= 4 else CAMS * behind + l
                    at = k * CAMS + l
                    out_ref[at : at + 1, lanes] = rows_ref[row : row + 1, :]


def whole_blocks(counts, shares, hot, other):
    return pl.pallas_call(
        blocks_body,
        out_shape=jax.ShapeDtypeStruct((CAMS * CAMS, CAM_DEV), F32),
        in_specs=[SMEM] + [VMEM] * 6,
        out_specs=VMEM,
        scratch_shapes=[pltpu.VMEM((BLOCK_ROWS, LANES), F32)],
        name="blocks",
    )(counts, *[near(x) for x in (*shares, hot, other)])


def order_body(core_ref, rows_ref, *refs):
    out_ref = refs[-1]
    width = SPAN * QUARTERS
    ends = out_ref.shape[1] // width
    for end in range(ends):
        source = pl.program_id(0) * ends + end
        for tile in range(width // LANES):
            at = end * width + tile * LANES
            out_ref[:, at : at + LANES] = rows_ref[source, tile * CAMS : (tile + 1) * CAMS, :]


def ordered(core, rows, before=None):
    ends, depth, lanes = rows.shape
    steps = 4
    width = ends // steps * depth // CAMS * lanes
    whole = jax.ShapeDtypeStruct((CAMS, 2 * steps * width), F32)
    in_specs = [VMEM]
    operands, aliases, flip = [core, near(rows)], {}, int(before is not None)
    if before is not None:
        in_specs.append(pl.BlockSpec(memory_space=pl.ANY))
        operands.append(before)
        aliases = {2: 0}
    return pl.pallas_call(
        order_body,
        grid_spec=pltpu.PrefetchScalarGridSpec(
            num_scalar_prefetch=1,
            grid=(steps,),
            in_specs=in_specs,
            out_specs=pl.BlockSpec((CAMS, width), lambda i, core: (0, jnp.bitwise_xor(core[0], flip) * steps + i)),
        ),
        out_shape=whole,
        input_output_aliases=aliases,
        name="order",
    )(*operands)


def exchanged(pieces, axes):
    return lax.all_to_all(pieces, axes, 0, 0, tiled=True)


def from_all(share, axes):
    count = lax.axis_size(axes)
    return exchanged(jnp.broadcast_to(share[None], (count, *share.shape)), axes)


def to_owner(share):
    pairs = [(level * 4 + column, column * 4 + level) for level in range(4) for column in range(4)]
    return lax.ppermute(share, ("zk", "x"), pairs)


def turned(share, axis, turn):
    count = lax.axis_size(axis)
    return lax.ppermute(share, axis, [(k, (k + turn) % count) for k in range(count)])


def local(jacobians, residuals, camera_local, bucket_counts, camera_map):
    targets = lax.axis_size(NEAR)
    level, core = lax.axis_index("zk"), lax.axis_index("c")
    cameras = camera_local.reshape(1, -1)
    sent = packed(jacobians, residuals, cameras, bucket_counts, targets)
    arrived = exchanged(sent.reshape(targets, -1, 4, LANES), NEAR).reshape(-1, LANES)
    camera_map, bucket_counts, arrived = lax.optimization_barrier((camera_map, bucket_counts, arrived))
    hot = jnp.argmax(bucket_counts[0])
    ids = camera_map.reshape(4, 2, 4, 2, QUARTERS, SPAN)
    ids = lax.dynamic_slice(ids, (0, 0, 0, core, level, 0), (4, 2, 4, 1, 1, SPAN))
    ids = ids.reshape(4, 8, SPAN).transpose(1, 0, 2).reshape(-1, 2, LANES)
    hot_ids = lax.dynamic_slice_in_dim(camera_map, hot * CAM_DEV + core * 4 * LANES, 4 * LANES)
    hot_ids = jnp.where(level == 0, hot_ids, -1).reshape(-1, 2, LANES)
    ids = jnp.concatenate([ids, hot_ids], axis=0)
    here = jnp.bitwise_and(jnp.right_shift(ids, 10), 31) == lax.axis_index(RANGE)
    codes = jnp.right_shift(ids, 15) * QUARTERS * SPAN + jnp.bitwise_and(ids, QUARTERS * SPAN - 1)
    codes = jnp.where(here & (ids >= 0), codes, -SPAN)
    sums = camera_sums(arrived)
    share = sums[0]
    for turn in range(1, QUARTERS):
        share = share + turned(sums[turn], "zk", turn)
    squares = to_owner(share[GRAD_ROWS:])
    slots = from_all(share[:GRAD_ROWS], RANGE)
    slots, squares = lax.optimization_barrier((slots, squares))
    shares = [squares] + [turned(squares, "x", turn) for turn in range(1, QUARTERS)]
    mine, theirs = placed(slots, codes, 2 * QUARTERS)
    own_hot = slots[:, 2 * CAMS : 2 * CAMS + HOT_ROWS]
    other_hot = turned(own_hot, "c", 1)
    mine = mine + turned(theirs, "c", 1)
    part = mine
    for turn in range(1, QUARTERS):
        part = part + turned(mine, "zk", turn)
    part, shares, other_hot = lax.optimization_barrier((part, shares, other_hot))
    blocks = whole_blocks(bucket_counts, shares, own_hot, other_hot)
    part = from_all(part, RANGE)
    part, blocks = lax.optimization_barrier((part, blocks))
    other = turned(part, "c", 1)
    core = core.reshape(1)
    gradient = ordered(core, part)
    gradient = ordered(core, other, gradient)
    return gradient, blocks


def solution(mesh):
    split = Mesh(mesh.devices.reshape(4, 2, 4, 2, mesh.shape["rep"]), ALL)
    return jax.shard_map(
        local,
        mesh=split,
        in_specs=(P(None, ALL), P(None, ALL), P(ALL), P(ALL, None), P()),
        out_specs=(P(), P(None, OBS)),
        check_vma=False,
    )
```

```python
import jax
import jax.numpy as jnp
from jax import lax
from jax.experimental import pallas as pl
from jax.experimental.pallas import tpu as pltpu
from jax.sharding import Mesh
from jax.sharding import PartitionSpec as P

CAM_DEV = 1024
HALF = 256
LANES = 128
SPAN = 256
QUARTERS = CAM_DEV // SPAN
CAMS = 9
PAIRS = 45
TERMS = 56
VALUES = 21
BLOCK = 26
HOT_ROWS = 7
HOT_FIRST = 5
GRAD_ROWS = 32
BLOCK_ROWS = 48
CHUNKS_PER_STEP = 4
OBS = ("zk", "zp", "y", "c")
ALL = ("zk", "zp", "y", "c", "x")
NEAR = ("zp", "y", "c", "x")
RANGE = ("zp", "y", "x")
F32 = jnp.float32
BF16 = jnp.bfloat16
VMEM = pl.BlockSpec(memory_space=pltpu.VMEM)
SMEM = pl.BlockSpec(memory_space=pltpu.SMEM)


def near(x):
    return pltpu.with_memory_space_constraint(x, pltpu.VMEM)


def two_pieces(x):
    upper = x.astype(BF16).astype(F32)
    return jnp.concatenate([upper, x - upper], axis=0).astype(BF16)


def kept_where(x, row, value):
    rows, lanes = x.shape
    kept = jnp.broadcast_to(row, (16, lanes)) == value
    kept = jnp.where(kept, 1.0, 0.0).astype(BF16)
    return (x.reshape(rows // 16, 16, lanes) * kept[None]).reshape(rows, lanes)


def one_hot(row):
    lanes = row.shape[1]
    spread = lax.broadcasted_iota(jnp.int32, (SPAN, lanes), 0) == row
    return jnp.where(spread, 1.0, 0.0).astype(BF16)


def product(left, right):
    return lax.dot_general(left, right, (((1,), (1,)), ((), ())), preferred_element_type=F32)


def set_operands(left_ref, right_ref, x, ids, parts, at):
    pieces = two_pieces(x)
    rows = pieces.shape[0]
    upper, lower = jnp.right_shift(ids, 8), jnp.bitwise_and(ids, SPAN - 1)
    for part in range(parts):
        left_ref[part * rows : (part + 1) * rows, at : at + LANES] = kept_where(pieces, upper, part)
    right_ref[:, at : at + LANES] = one_hot(lower)


def pack_body(
    counts_ref, jac_ref, res_ref, cam_ref, out_ref, kept_ref, terms_ref, left_ref, right_ref
):
    targets = out_ref.shape[0] // (2 * BLOCK)
    capacity = jac_ref.shape[1] // 16
    step = pl.program_id(0)
    for level in range(4):

        @pl.when(step == level)
        def _():
            for side in range(2):
                for owner in range(8):
                    bucket = side * 8 + owner
                    count = counts_ref[0, level * 16 + bucket]
                    target = side * 32 + owner * 4 + level
                    for half in range(2):
                        at = bucket * capacity + half * LANES
                        here = slice(at, at + LANES)
                        live = lax.broadcasted_iota(jnp.int32, (1, LANES), 1) + half * LANES < count
                        row = (2 * target + half) * BLOCK
                        out_ref[row : row + 18, :] = jnp.where(live, jac_ref[:, here], 0.0)
                        out_ref[row + 18 : row + 20, :] = jnp.where(live, res_ref[:, here], 0.0)
                        out_ref[row + 20 : row + 21, :] = cam_ref[:, here].astype(F32)

    hot = jnp.int32(-1)
    for bucket in range(16):
        hot = jnp.where(counts_ref[0, step * 16 + bucket] > HALF, bucket, hot)

    @pl.when(hot >= 0)
    def _():
        count = counts_ref[0, step * 16 + hot]
        for half in range(2):
            at = pl.multiple_of(hot * capacity + HALF + half * LANES, LANES)
            here = pl.ds(at, LANES)
            live = lax.broadcasted_iota(jnp.int32, (1, LANES), 1) + HALF + half * LANES < count
            kept_ref[half, :18, :] = jnp.where(live, jac_ref[:, here], 0.0)
            kept_ref[half, 18:20, :] = jnp.where(live, res_ref[:, here], 0.0)
            kept_ref[half, 20:21, :] = cam_ref[:, here].astype(F32)

    @pl.when(step == pl.num_programs(0) - 1)
    def _():
        for half in range(2):
            kept = kept_ref[half]
            first, second = kept[:CAMS], kept[CAMS : 2 * CAMS]
            for turn in range(5):
                around = first if turn == 0 else jnp.concatenate([first[turn:], first[:turn]], axis=0)
                beside = second if turn == 0 else jnp.concatenate([second[turn:], second[:turn]], axis=0)
                terms_ref[CAMS * turn : CAMS * (turn + 1), :] = first * around + second * beside
            terms_ref[PAIRS : PAIRS + CAMS, :] = first * kept[18:19] + second * kept[19:20]
            terms_ref[PAIRS + CAMS : TERMS, :] = jnp.zeros((TERMS - PAIRS - CAMS, LANES), F32)
            ids = kept[20:21].astype(jnp.int32)
            set_operands(left_ref, right_ref, terms_ref[...], ids, QUARTERS, half * LANES)
        summed = product(left_ref[...], right_ref[...])
        for share in range(targets):
            rows, column = HOT_ROWS * (share // 8), LANES * (share % 8)
            start = 2 * TERMS * (column // SPAN) + rows
            lanes = slice(column % SPAN, column % SPAN + LANES)
            piece = (
                summed[start : start + HOT_ROWS, lanes]
                + summed[start + TERMS : start + TERMS + HOT_ROWS, lanes]
            )
            row = 2 * share * BLOCK + VALUES
            out_ref[row : row + HOT_FIRST, :] = piece[:HOT_FIRST]
            row += BLOCK
            out_ref[row : row + HOT_ROWS - HOT_FIRST, :] = piece[HOT_FIRST:]


def packed(jacobians, residuals, cameras, counts, targets):
    steps = 4
    width = jacobians.shape[1] // steps
    return pl.pallas_call(
        pack_body,
        grid=(steps,),
        out_shape=pltpu.VMEM((targets * 2 * BLOCK, LANES), F32),
        in_specs=[
            SMEM,
            pl.BlockSpec((18, width), lambda i: (0, i)),
            pl.BlockSpec((2, width), lambda i: (0, i)),
            pl.BlockSpec((1, width), lambda i: (0, i)),
        ],
        out_specs=VMEM,
        scratch_shapes=[
            pltpu.VMEM((2, 24, LANES), F32),
            pltpu.VMEM((TERMS, LANES), F32),
            pltpu.VMEM((2 * TERMS * QUARTERS, 2 * LANES), BF16),
            pltpu.VMEM((SPAN, 2 * LANES), BF16),
        ],
        name="pack",
    )(counts, jacobians, residuals, cameras)


def sums_body(arrived_ref, *refs):
    out_refs, (terms_ref, left_ref, right_ref, acc_ref, hot_ref) = refs[:QUARTERS], refs[QUARTERS:]
    step = pl.program_id(0)

    @pl.when(step == 0)
    def _():
        acc_ref[...] = jnp.zeros_like(acc_ref)
        terms_ref[...] = jnp.zeros_like(terms_ref)
        hot_ref[...] = jnp.zeros_like(hot_ref)

    for chunk in range(CHUNKS_PER_STEP):
        start = chunk * 8 * BLOCK
        value = [arrived_ref[pl.ds(start + row, 8, stride=BLOCK), :] for row in range(VALUES)]
        for turn in range(5):
            for k in range(CAMS):
                other = (k + turn) % CAMS
                term = value[k] * value[other] + value[CAMS + k] * value[CAMS + other]
                terms_ref[chunk, pl.ds(CAMS * turn + k, 8, stride=TERMS), :] = term
        for k in range(CAMS):
            term = value[k] * value[18] + value[CAMS + k] * value[19]
            terms_ref[chunk, pl.ds(PAIRS + k, 8, stride=TERMS), :] = term
        ids = value[20].astype(jnp.int32)
        for group in range(8):
            x = terms_ref[chunk, group * TERMS : (group + 1) * TERMS, :]
            row = ids[group : group + 1, :]
            set_operands(left_ref.at[chunk], right_ref.at[chunk], x, row, QUARTERS, group * LANES)
        for source in range(4):
            row = start + 2 * source * BLOCK + VALUES
            hot_ref[:HOT_FIRST, :] += arrived_ref[row : row + HOT_FIRST, :]
            row += BLOCK
            rest = HOT_ROWS - HOT_FIRST
            hot_ref[HOT_FIRST:HOT_ROWS, :] += arrived_ref[row : row + rest, :]
        acc_ref[...] += product(left_ref[chunk], right_ref[chunk])

    @pl.when(step == pl.num_programs(0) - 1)
    def _():
        for turn, out_ref in enumerate(out_refs):
            part = lax.rem(lax.axis_index("zk") + turn, QUARTERS)
            upper = pl.ds(pl.multiple_of(2 * TERMS * part, 16), TERMS)
            lower = pl.ds(pl.multiple_of(2 * TERMS * part + TERMS, 8), TERMS)
            both = acc_ref[upper, :] + acc_ref[lower, :]
            for half in range(2):
                lanes = slice(half * LANES, (half + 1) * LANES)
                at = GRAD_ROWS + half * BLOCK_ROWS
                out_ref[at : at + BLOCK_ROWS, :] = both[:BLOCK_ROWS, lanes]
                out_ref[half * CAMS : (half + 1) * CAMS, :] = both[PAIRS : PAIRS + CAMS, lanes]
            out_ref[2 * CAMS : 2 * CAMS + HOT_ROWS, :] = hot_ref[:HOT_ROWS]
            rest = GRAD_ROWS - 2 * CAMS - HOT_ROWS
            out_ref[GRAD_ROWS - rest : GRAD_ROWS, :] = jnp.zeros((rest, LANES), F32)


def camera_sums(arrived):
    rows = arrived.shape[0]
    depth = 8 * LANES
    step = 8 * BLOCK * CHUNKS_PER_STEP
    out = (GRAD_ROWS + 2 * BLOCK_ROWS, LANES)
    return pl.pallas_call(
        sums_body,
        grid=(rows // step,),
        out_shape=[pltpu.VMEM(out, F32)] * QUARTERS,
        in_specs=[pl.BlockSpec((step, LANES), lambda i: (i, 0))],
        out_specs=[VMEM] * QUARTERS,
        scratch_shapes=[
            pltpu.VMEM((CHUNKS_PER_STEP, 8 * TERMS, LANES), F32),
            pltpu.VMEM((CHUNKS_PER_STEP, 2 * TERMS * QUARTERS, depth), BF16),
            pltpu.VMEM((CHUNKS_PER_STEP, SPAN, depth), BF16),
            pltpu.VMEM((2 * TERMS * QUARTERS, SPAN), F32),
            pltpu.VMEM((8, LANES), F32),
        ],
        compiler_params=pltpu.CompilerParams(vmem_limit_bytes=40 << 20),
        cost_estimate=pl.CostEstimate(
            flops=2 * 2 * TERMS * CAM_DEV * 128 * rows // BLOCK, transcendentals=0, bytes_accessed=rows * 512
        ),
        name="sums",
    )(near(arrived))


def place_body(slots_ref, codes_ref, mine_ref, theirs_ref, left_ref, right_ref, acc_ref):
    sources = slots_ref.shape[0]
    ranges = acc_ref.shape[0] // 32
    blank = jnp.zeros((16 - CAMS, LANES), F32)

    def set_group(x, codes, chunk, group):
        x = jnp.concatenate([x, blank], axis=0)
        set_operands(left_ref.at[chunk], right_ref.at[chunk], x, codes, ranges, group * LANES)

    for chunk in range(sources // 4):
        for group in range(8):
            source, half = chunk * 4 + group // 2, group % 2
            x = slots_ref[source, half * CAMS : (half + 1) * CAMS, :]
            set_group(x, codes_ref[source, half : half + 1, :], chunk, group)
        summed = product(left_ref[chunk], right_ref[chunk])
        acc_ref[...] = summed if chunk == 0 else acc_ref[...] + summed
    split = HOT_ROWS - PAIRS % HOT_ROWS
    for group in range(4):
        source = PAIRS // HOT_ROWS * 4 + group
        x = slots_ref[source, 2 * CAMS + HOT_ROWS - split : 2 * CAMS + HOT_ROWS, :]
        rest = slots_ref[source + 4, 2 * CAMS : 3 * CAMS - split, :]
        x = jnp.concatenate([x, rest], axis=0)
        set_group(x, codes_ref[sources + group // 2, group % 2 : group % 2 + 1, :], sources // 4, group)
    depth = 4 * LANES
    acc_ref[...] += product(left_ref[sources // 4, :, :depth], right_ref[sources // 4, :, :depth])
    for flip, out_ref in enumerate((mine_ref, theirs_ref)):
        core = jnp.bitwise_xor(lax.axis_index("c"), flip)
        for part in range(QUARTERS):
            at = pl.multiple_of((core * QUARTERS + part) * 32, 32)
            both = acc_ref[pl.ds(at, CAMS), :] + acc_ref[pl.ds(at + 16, CAMS), :]
            for half in range(2):
                row = (part * 2 + half) * CAMS
                out_ref[row : row + CAMS, :] = both[:, half * LANES : (half + 1) * LANES]
    base = ranges * CAMS
    for source in range(sources):
        row = base + source * HOT_ROWS
        theirs_ref[row : row + HOT_ROWS, :] = slots_ref[source, 2 * CAMS : 2 * CAMS + HOT_ROWS, :]


def placed(slots, codes, ranges):
    depth = 8 * LANES
    chunks = slots.shape[0] // 4 + 1
    return pl.pallas_call(
        place_body,
        out_shape=[
            pltpu.VMEM((ranges * CAMS, LANES), F32),
            pltpu.VMEM((ranges * CAMS + slots.shape[0] * HOT_ROWS, LANES), F32),
        ],
        in_specs=[VMEM, VMEM],
        out_specs=[VMEM, VMEM],
        scratch_shapes=[
            pltpu.VMEM((chunks, 32 * ranges, depth), BF16),
            pltpu.VMEM((chunks, SPAN, depth), BF16),
            pltpu.VMEM((32 * ranges, SPAN), F32),
        ],
        name="place",
    )(near(slots), near(codes))


def blocks_body(counts_ref, one_ref, two_ref, three_ref, four_ref, hot_ref, other_ref, out_ref, rows_ref):
    column, core = lax.axis_index("x"), lax.axis_index("c")
    own = jnp.where(counts_ref[0, lax.axis_index(OBS)] > HALF, 1, 0)
    for turn, share_ref in enumerate((one_ref, two_ref, three_ref, four_ref)):
        part = lax.rem(column - turn + QUARTERS, QUARTERS)
        for half in range(2):
            for group in range(TERMS // HOT_ROWS):
                start, stop = HOT_ROWS * group, min(HOT_ROWS * (group + 1), PAIRS)
                if start >= PAIRS:
                    continue
                source = group * 4 + lax.rem(part, 2) * 2 + half
                here = hot_ref[source, 2 * CAMS : 2 * CAMS + stop - start, :]
                row = 2 * CAMS * QUARTERS + source * HOT_ROWS
                there = other_ref[pl.ds(row, stop - start), :]
                hot = jnp.where(lax.div(part, 2) == core, here, there)
                share = share_ref[half * BLOCK_ROWS + start : half * BLOCK_ROWS + stop, :]
                rows_ref[start:stop, :] = share + jnp.where(own > 0, hot, 0.0)
            lanes = pl.ds(pl.multiple_of((part * 2 + half) * LANES, LANES), LANES)
            for k in range(CAMS):
                for l in range(CAMS):
                    ahead, behind = (l - k) % CAMS, (k - l) % CAMS
                    row = CAMS * ahead + k if ahead <= 4 else CAMS * behind + l
                    at = k * CAMS + l
                    out_ref[at : at + 1, lanes] = rows_ref[row : row + 1, :]


def whole_blocks(counts, shares, hot, other):
    return pl.pallas_call(
        blocks_body,
        out_shape=jax.ShapeDtypeStruct((CAMS * CAMS, CAM_DEV), F32),
        in_specs=[SMEM] + [VMEM] * 6,
        out_specs=VMEM,
        scratch_shapes=[pltpu.VMEM((BLOCK_ROWS, LANES), F32)],
        name="blocks",
    )(counts, *[near(x) for x in (*shares, hot, other)])


def order_body(core_ref, rows_ref, *refs):
    out_ref = refs[-1]
    width = SPAN * QUARTERS
    ends = out_ref.shape[1] // width
    for end in range(ends):
        source = pl.program_id(0) * ends + end
        for tile in range(width // LANES):
            at = end * width + tile * LANES
            out_ref[:, at : at + LANES] = rows_ref[source, tile * CAMS : (tile + 1) * CAMS, :]


def ordered(core, rows, before=None):
    ends, depth, lanes = rows.shape
    steps = 4
    width = ends // steps * depth // CAMS * lanes
    whole = jax.ShapeDtypeStruct((CAMS, 2 * steps * width), F32)
    in_specs = [VMEM]
    operands, aliases, flip = [core, near(rows)], {}, int(before is not None)
    if before is not None:
        in_specs.append(pl.BlockSpec(memory_space=pl.ANY))
        operands.append(before)
        aliases = {2: 0}
    return pl.pallas_call(
        order_body,
        grid_spec=pltpu.PrefetchScalarGridSpec(
            num_scalar_prefetch=1,
            grid=(steps,),
            in_specs=in_specs,
            out_specs=pl.BlockSpec((CAMS, width), lambda i, core: (0, jnp.bitwise_xor(core[0], flip) * steps + i)),
        ),
        out_shape=whole,
        input_output_aliases=aliases,
        name="order",
    )(*operands)


def exchanged(pieces, axes):
    return lax.all_to_all(pieces, axes, 0, 0, tiled=True)


def from_all(share, axes):
    count = lax.axis_size(axes)
    return exchanged(jnp.broadcast_to(share[None], (count, *share.shape)), axes)


def to_owner(share):
    pairs = [(level * 4 + column, column * 4 + level) for level in range(4) for column in range(4)]
    return lax.ppermute(share, ("zk", "x"), pairs)


def turned(share, axis, turn):
    count = lax.axis_size(axis)
    return lax.ppermute(share, axis, [(k, (k + turn) % count) for k in range(count)])


def local(jacobians, residuals, camera_local, bucket_counts, camera_map):
    targets = lax.axis_size(NEAR)
    level, core = lax.axis_index("zk"), lax.axis_index("c")
    cameras = camera_local.reshape(1, -1)
    sent = packed(jacobians, residuals, cameras, bucket_counts, targets)
    arrived = exchanged(sent.reshape(targets, -1, 4, LANES), NEAR).reshape(-1, LANES)
    camera_map, bucket_counts, arrived = lax.optimization_barrier((camera_map, bucket_counts, arrived))
    hot = jnp.argmax(bucket_counts[0])
    ids = camera_map.reshape(4, 2, 4, 2, QUARTERS, SPAN)
    ids = lax.dynamic_slice(ids, (0, 0, 0, core, level, 0), (4, 2, 4, 1, 1, SPAN))
    ids = ids.reshape(4, 8, SPAN).transpose(1, 0, 2).reshape(-1, 2, LANES)
    hot_ids = lax.dynamic_slice_in_dim(camera_map, hot * CAM_DEV + core * 4 * LANES, 4 * LANES)
    hot_ids = jnp.where(level == 0, hot_ids, -1).reshape(-1, 2, LANES)
    ids = jnp.concatenate([ids, hot_ids], axis=0)
    here = jnp.bitwise_and(jnp.right_shift(ids, 10), 31) == lax.axis_index(RANGE)
    codes = jnp.right_shift(ids, 15) * QUARTERS * SPAN + jnp.bitwise_and(ids, QUARTERS * SPAN - 1)
    codes = jnp.where(here & (ids >= 0), codes, -SPAN)
    sums = camera_sums(arrived)
    share = sums[0]
    for turn in range(1, QUARTERS):
        share = share + turned(sums[turn], "zk", turn)
    squares = to_owner(share[GRAD_ROWS:])
    slots = from_all(share[:GRAD_ROWS], RANGE)
    slots, squares = lax.optimization_barrier((slots, squares))
    shares = [squares] + [turned(squares, "x", turn) for turn in range(1, QUARTERS)]
    mine, theirs = placed(slots, codes, 2 * QUARTERS)
    theirs = turned(theirs, "c", 1)
    mine = mine + theirs[: mine.shape[0]]
    part = mine
    for turn in range(1, QUARTERS):
        part = part + turned(mine, "zk", turn)
    part, shares = lax.optimization_barrier((part, shares))
    blocks = whole_blocks(bucket_counts, shares, slots, theirs)
    part = from_all(part, RANGE)
    part, blocks = lax.optimization_barrier((part, blocks))
    other = turned(part, "c", 1)
    core = core.reshape(1)
    gradient = ordered(core, part)
    gradient = ordered(core, other, gradient)
    return gradient, blocks


def solution(mesh):
    split = Mesh(mesh.devices.reshape(4, 2, 4, 2, mesh.shape["rep"]), ALL)
    return jax.shard_map(
        local,
        mesh=split,
        in_specs=(P(None, ALL), P(None, ALL), P(ALL), P(ALL, None), P()),
        out_specs=(P(), P(None, OBS)),
        check_vma=False,
    )
```

```python
import jax
import jax.numpy as jnp
from jax import lax
from jax.experimental import pallas as pl
from jax.experimental.pallas import tpu as pltpu
from jax.sharding import Mesh
from jax.sharding import PartitionSpec as P


CAM_DEV = 1024
HALF = 256
LANES = 128
SPAN = 256
QUARTERS = CAM_DEV // SPAN
CAMS = 9
PAIRS = 45
TERMS = 56
VALUES = 21
BLOCK = 26
HOT_ROWS = 7
HOT_FIRST = 5
GRAD_ROWS = 32
BLOCK_ROWS = 48
CHUNKS_PER_STEP = 4
OBS = ("zk", "zp", "y", "c")
ALL = ("zk", "zp", "y", "c", "x")
NEAR = ("zp", "y", "c", "x")
RANGE = ("zp", "y", "x")
F32 = jnp.float32
BF16 = jnp.bfloat16
VMEM = pl.BlockSpec(memory_space=pltpu.VMEM)
SMEM = pl.BlockSpec(memory_space=pltpu.SMEM)


def near(x):
    return pltpu.with_memory_space_constraint(x, pltpu.VMEM)


def two_pieces(x):
    upper = x.astype(BF16).astype(F32)
    return jnp.concatenate([upper, x - upper], axis=0).astype(BF16)


def kept_where(x, row, value):
    rows, lanes = x.shape
    kept = jnp.broadcast_to(row, (16, lanes)) == value
    kept = jnp.where(kept, 1.0, 0.0).astype(BF16)
    return (x.reshape(rows // 16, 16, lanes) * kept[None]).reshape(rows, lanes)


def one_hot(row):
    lanes = row.shape[1]
    spread = lax.broadcasted_iota(jnp.int32, (SPAN, lanes), 0) == row
    return jnp.where(spread, 1.0, 0.0).astype(BF16)


def product(left, right):
    return lax.dot_general(left, right, (((1,), (1,)), ((), ())), preferred_element_type=F32)


def set_operands(left_ref, right_ref, x, ids, parts, at):
    pieces = two_pieces(x)
    rows = pieces.shape[0]
    upper, lower = jnp.right_shift(ids, 8), jnp.bitwise_and(ids, SPAN - 1)
    for part in range(parts):
        left_ref[part * rows : (part + 1) * rows, at : at + LANES] = kept_where(pieces, upper, part)
    right_ref[:, at : at + LANES] = one_hot(lower)


def pack_body(
    counts_ref, jac_ref, res_ref, cam_ref, out_ref, kept_ref, terms_ref, left_ref, right_ref
):
    targets = out_ref.shape[0] // (2 * BLOCK)
    capacity = jac_ref.shape[1] // 16
    step = pl.program_id(0)
    for level in range(4):

        @pl.when(step == level)
        def _():
            for side in range(2):
                for owner in range(8):
                    bucket = side * 8 + owner
                    count = counts_ref[0, level * 16 + bucket]
                    target = side * 32 + owner * 4 + level
                    for half in range(2):
                        at = bucket * capacity + half * LANES
                        here = slice(at, at + LANES)
                        live = lax.broadcasted_iota(jnp.int32, (1, LANES), 1) + half * LANES < count
                        row = (2 * target + half) * BLOCK
                        out_ref[row : row + 18, :] = jnp.where(live, jac_ref[:, here], 0.0)
                        out_ref[row + 18 : row + 20, :] = jnp.where(live, res_ref[:, here], 0.0)
                        out_ref[row + 20 : row + 21, :] = cam_ref[:, here].astype(F32)

    hot = jnp.int32(-1)
    for bucket in range(16):
        hot = jnp.where(counts_ref[0, step * 16 + bucket] > HALF, bucket, hot)

    @pl.when(hot >= 0)
    def _():
        count = counts_ref[0, step * 16 + hot]
        for half in range(2):
            at = pl.multiple_of(hot * capacity + HALF + half * LANES, LANES)
            here = pl.ds(at, LANES)
            live = lax.broadcasted_iota(jnp.int32, (1, LANES), 1) + HALF + half * LANES < count
            kept_ref[half, :18, :] = jnp.where(live, jac_ref[:, here], 0.0)
            kept_ref[half, 18:20, :] = jnp.where(live, res_ref[:, here], 0.0)
            kept_ref[half, 20:21, :] = cam_ref[:, here].astype(F32)

    @pl.when(step == pl.num_programs(0) - 1)
    def _():
        for half in range(2):
            kept = kept_ref[half]
            first, second = kept[:CAMS], kept[CAMS : 2 * CAMS]
            for turn in range(5):
                around = first if turn == 0 else jnp.concatenate([first[turn:], first[:turn]], axis=0)
                beside = second if turn == 0 else jnp.concatenate([second[turn:], second[:turn]], axis=0)
                terms_ref[CAMS * turn : CAMS * (turn + 1), :] = first * around + second * beside
            terms_ref[PAIRS : PAIRS + CAMS, :] = first * kept[18:19] + second * kept[19:20]
            terms_ref[PAIRS + CAMS : TERMS, :] = jnp.zeros((TERMS - PAIRS - CAMS, LANES), F32)
            ids = kept[20:21].astype(jnp.int32)
            set_operands(left_ref, right_ref, terms_ref[...], ids, QUARTERS, half * LANES)
        summed = product(left_ref[...], right_ref[...])
        for share in range(targets):
            rows, column = HOT_ROWS * (share // 8), LANES * (share % 8)
            start = 2 * TERMS * (column // SPAN) + rows
            lanes = slice(column % SPAN, column % SPAN + LANES)
            piece = (
                summed[start : start + HOT_ROWS, lanes]
                + summed[start + TERMS : start + TERMS + HOT_ROWS, lanes]
            )
            row = 2 * share * BLOCK + VALUES
            out_ref[row : row + HOT_FIRST, :] = piece[:HOT_FIRST]
            row += BLOCK
            out_ref[row : row + HOT_ROWS - HOT_FIRST, :] = piece[HOT_FIRST:]


def packed(jacobians, residuals, cameras, counts, targets):
    steps = 4
    width = jacobians.shape[1] // steps
    return pl.pallas_call(
        pack_body,
        grid=(steps,),
        out_shape=pltpu.VMEM((targets * 2 * BLOCK, LANES), F32),
        in_specs=[
            SMEM,
            pl.BlockSpec((18, width), lambda i: (0, i)),
            pl.BlockSpec((2, width), lambda i: (0, i)),
            pl.BlockSpec((1, width), lambda i: (0, i)),
        ],
        out_specs=VMEM,
        scratch_shapes=[
            pltpu.VMEM((2, 24, LANES), F32),
            pltpu.VMEM((TERMS, LANES), F32),
            pltpu.VMEM((2 * TERMS * QUARTERS, 2 * LANES), BF16),
            pltpu.VMEM((SPAN, 2 * LANES), BF16),
        ],
        name="pack",
    )(counts, jacobians, residuals, cameras)


def sums_body(arrived_ref, *refs):
    out_refs, (terms_ref, left_ref, right_ref, acc_ref, hot_ref) = refs[:QUARTERS], refs[QUARTERS:]
    step = pl.program_id(0)

    @pl.when(step == 0)
    def _():
        acc_ref[...] = jnp.zeros_like(acc_ref)
        terms_ref[...] = jnp.zeros_like(terms_ref)
        hot_ref[...] = jnp.zeros_like(hot_ref)

    for chunk in range(CHUNKS_PER_STEP):
        start = chunk * 8 * BLOCK
        value = [arrived_ref[pl.ds(start + row, 8, stride=BLOCK), :] for row in range(VALUES)]
        for turn in range(5):
            for k in range(CAMS):
                other = (k + turn) % CAMS
                term = value[k] * value[other] + value[CAMS + k] * value[CAMS + other]
                terms_ref[chunk, pl.ds(CAMS * turn + k, 8, stride=TERMS), :] = term
        for k in range(CAMS):
            term = value[k] * value[18] + value[CAMS + k] * value[19]
            terms_ref[chunk, pl.ds(PAIRS + k, 8, stride=TERMS), :] = term
        ids = value[20].astype(jnp.int32)
        for group in range(8):
            x = terms_ref[chunk, group * TERMS : (group + 1) * TERMS, :]
            row = ids[group : group + 1, :]
            set_operands(left_ref.at[chunk], right_ref.at[chunk], x, row, QUARTERS, group * LANES)
        for source in range(4):
            row = start + 2 * source * BLOCK + VALUES
            hot_ref[:HOT_FIRST, :] += arrived_ref[row : row + HOT_FIRST, :]
            row += BLOCK
            rest = HOT_ROWS - HOT_FIRST
            hot_ref[HOT_FIRST:HOT_ROWS, :] += arrived_ref[row : row + rest, :]
        acc_ref[...] += product(left_ref[chunk], right_ref[chunk])

    @pl.when(step == pl.num_programs(0) - 1)
    def _():
        for turn, out_ref in enumerate(out_refs):
            part = lax.rem(lax.axis_index("zk") + turn, QUARTERS)
            upper = pl.ds(pl.multiple_of(2 * TERMS * part, 16), TERMS)
            lower = pl.ds(pl.multiple_of(2 * TERMS * part + TERMS, 8), TERMS)
            both = acc_ref[upper, :] + acc_ref[lower, :]
            for half in range(2):
                lanes = slice(half * LANES, (half + 1) * LANES)
                at = GRAD_ROWS + half * BLOCK_ROWS
                out_ref[at : at + BLOCK_ROWS, :] = both[:BLOCK_ROWS, lanes]
                out_ref[half * CAMS : (half + 1) * CAMS, :] = both[PAIRS : PAIRS + CAMS, lanes]
            out_ref[2 * CAMS : 2 * CAMS + HOT_ROWS, :] = hot_ref[:HOT_ROWS]
            rest = GRAD_ROWS - 2 * CAMS - HOT_ROWS
            out_ref[GRAD_ROWS - rest : GRAD_ROWS, :] = jnp.zeros((rest, LANES), F32)


def camera_sums(arrived):
    rows = arrived.shape[0]
    depth = 8 * LANES
    step = 8 * BLOCK * CHUNKS_PER_STEP
    out = (GRAD_ROWS + 2 * BLOCK_ROWS, LANES)
    return pl.pallas_call(
        sums_body,
        grid=(rows // step,),
        out_shape=[pltpu.VMEM(out, F32)] * QUARTERS,
        in_specs=[pl.BlockSpec((step, LANES), lambda i: (i, 0))],
        out_specs=[VMEM] * QUARTERS,
        scratch_shapes=[
            pltpu.VMEM((CHUNKS_PER_STEP, 8 * TERMS, LANES), F32),
            pltpu.VMEM((CHUNKS_PER_STEP, 2 * TERMS * QUARTERS, depth), BF16),
            pltpu.VMEM((CHUNKS_PER_STEP, SPAN, depth), BF16),
            pltpu.VMEM((2 * TERMS * QUARTERS, SPAN), F32),
            pltpu.VMEM((8, LANES), F32),
        ],
        compiler_params=pltpu.CompilerParams(vmem_limit_bytes=40 << 20),
        cost_estimate=pl.CostEstimate(
            flops=2 * 2 * TERMS * CAM_DEV * 128 * rows // BLOCK, transcendentals=0, bytes_accessed=rows * 512
        ),
        name="sums",
    )(near(arrived))


def place_body(slots_ref, codes_ref, mine_ref, theirs_ref, left_ref, right_ref, acc_ref):
    sources = slots_ref.shape[0]
    ranges = acc_ref.shape[0] // 32
    blank = jnp.zeros((16 - CAMS, LANES), F32)

    def set_group(x, codes, chunk, group):
        x = jnp.concatenate([x, blank], axis=0)
        set_operands(left_ref.at[chunk], right_ref.at[chunk], x, codes, ranges, group * LANES)

    for chunk in range(sources // 4):
        for group in range(8):
            source, half = chunk * 4 + group // 2, group % 2
            x = slots_ref[source, half * CAMS : (half + 1) * CAMS, :]
            set_group(x, codes_ref[source, half : half + 1, :], chunk, group)
        summed = product(left_ref[chunk], right_ref[chunk])
        acc_ref[...] = summed if chunk == 0 else acc_ref[...] + summed
    split = HOT_ROWS - PAIRS % HOT_ROWS
    for group in range(4):
        source = PAIRS // HOT_ROWS * 4 + group
        x = slots_ref[source, 2 * CAMS + HOT_ROWS - split : 2 * CAMS + HOT_ROWS, :]
        rest = slots_ref[source + 4, 2 * CAMS : 3 * CAMS - split, :]
        x = jnp.concatenate([x, rest], axis=0)
        set_group(x, codes_ref[sources + group // 2, group % 2 : group % 2 + 1, :], sources // 4, group)
    depth = 4 * LANES
    acc_ref[...] += product(left_ref[sources // 4, :, :depth], right_ref[sources // 4, :, :depth])
    for flip, out_ref in enumerate((mine_ref, theirs_ref)):
        core = jnp.bitwise_xor(lax.axis_index("c"), flip)
        for part in range(QUARTERS):
            at = pl.multiple_of((core * QUARTERS + part) * 32, 32)
            both = acc_ref[pl.ds(at, CAMS), :] + acc_ref[pl.ds(at + 16, CAMS), :]
            for half in range(2):
                row = (part * 2 + half) * CAMS
                out_ref[row : row + CAMS, :] = both[:, half * LANES : (half + 1) * LANES]
    base = ranges * CAMS
    for source in range(sources):
        row = base + source * HOT_ROWS
        theirs_ref[row : row + HOT_ROWS, :] = slots_ref[source, 2 * CAMS : 2 * CAMS + HOT_ROWS, :]


def placed(slots, codes, ranges):
    depth = 8 * LANES
    chunks = slots.shape[0] // 4 + 1
    return pl.pallas_call(
        place_body,
        out_shape=[
            pltpu.VMEM((ranges * CAMS, LANES), F32),
            pltpu.VMEM((ranges * CAMS + slots.shape[0] * HOT_ROWS, LANES), F32),
        ],
        in_specs=[VMEM, VMEM],
        out_specs=[VMEM, VMEM],
        scratch_shapes=[
            pltpu.VMEM((chunks, 32 * ranges, depth), BF16),
            pltpu.VMEM((chunks, SPAN, depth), BF16),
            pltpu.VMEM((32 * ranges, SPAN), F32),
        ],
        name="place",
    )(near(slots), near(codes))


def blocks_body(counts_ref, one_ref, two_ref, three_ref, four_ref, hot_ref, other_ref, out_ref, rows_ref):
    column, core = lax.axis_index("x"), lax.axis_index("c")
    own = jnp.where(counts_ref[0, lax.axis_index(OBS)] > HALF, 1, 0)
    for turn, share_ref in enumerate((one_ref, two_ref, three_ref, four_ref)):
        part = lax.rem(column - turn + QUARTERS, QUARTERS)
        for half in range(2):
            for group in range(TERMS // HOT_ROWS):
                start, stop = HOT_ROWS * group, min(HOT_ROWS * (group + 1), PAIRS)
                if start >= PAIRS:
                    continue
                source = group * 4 + lax.rem(part, 2) * 2 + half
                here = hot_ref[source, 2 * CAMS : 2 * CAMS + stop - start, :]
                row = 2 * CAMS * QUARTERS + source * HOT_ROWS
                there = other_ref[pl.ds(row, stop - start), :]
                hot = jnp.where(lax.div(part, 2) == core, here, there)
                share = share_ref[half * BLOCK_ROWS + start : half * BLOCK_ROWS + stop, :]
                rows_ref[start:stop, :] = share + jnp.where(own > 0, hot, 0.0)
            lanes = pl.ds(pl.multiple_of((part * 2 + half) * LANES, LANES), LANES)
            for k in range(CAMS):
                for l in range(CAMS):
                    ahead, behind = (l - k) % CAMS, (k - l) % CAMS
                    row = CAMS * ahead + k if ahead <= 4 else CAMS * behind + l
                    at = k * CAMS + l
                    out_ref[at : at + 1, lanes] = rows_ref[row : row + 1, :]


def whole_blocks(counts, shares, hot, other):
    return pl.pallas_call(
        blocks_body,
        out_shape=jax.ShapeDtypeStruct((CAMS * CAMS, CAM_DEV), F32),
        in_specs=[SMEM] + [VMEM] * 6,
        out_specs=VMEM,
        scratch_shapes=[pltpu.VMEM((BLOCK_ROWS, LANES), F32)],
        name="blocks",
    )(counts, *[near(x) for x in (*shares, hot, other)])


def order_body(core_ref, rows_ref, *refs):
    out_ref = refs[-1]
    width = SPAN * QUARTERS
    ends = out_ref.shape[1] // width
    for end in range(ends):
        source = pl.program_id(0) * ends + end
        for tile in range(width // LANES):
            at = end * width + tile * LANES
            out_ref[:, at : at + LANES] = rows_ref[source, tile * CAMS : (tile + 1) * CAMS, :]


def ordered(core, rows, before=None):
    ends, depth, lanes = rows.shape
    steps = 4
    width = ends // steps * depth // CAMS * lanes
    whole = jax.ShapeDtypeStruct((CAMS, 2 * steps * width), F32)
    in_specs = [VMEM]
    operands, aliases, flip = [core, near(rows)], {}, int(before is not None)
    if before is not None:
        in_specs.append(pl.BlockSpec(memory_space=pl.ANY))
        operands.append(before)
        aliases = {2: 0}
    return pl.pallas_call(
        order_body,
        grid_spec=pltpu.PrefetchScalarGridSpec(
            num_scalar_prefetch=1,
            grid=(steps,),
            in_specs=in_specs,
            out_specs=pl.BlockSpec((CAMS, width), lambda i, core: (0, jnp.bitwise_xor(core[0], flip) * steps + i)),
        ),
        out_shape=whole,
        input_output_aliases=aliases,
        name="order",
    )(*operands)


def exchanged(pieces, axes):
    return lax.all_to_all(pieces, axes, 0, 0, tiled=True)


def from_all(share, axes):
    count = lax.axis_size(axes)
    return exchanged(jnp.broadcast_to(share[None], (count, *share.shape)), axes)


def to_owner(share):
    pairs = [(level * 4 + column, column * 4 + level) for level in range(4) for column in range(4)]
    return lax.ppermute(share, ("zk", "x"), pairs)


def turned(share, axis, turn):
    count = lax.axis_size(axis)
    return lax.ppermute(share, axis, [(k, (k + turn) % count) for k in range(count)])


def local(jacobians, residuals, camera_local, bucket_counts, camera_map):
    targets = lax.axis_size(NEAR)
    level, core = lax.axis_index("zk"), lax.axis_index("c")
    cameras = camera_local.reshape(1, -1)
    sent = packed(jacobians, residuals, cameras, bucket_counts, targets)
    arrived = exchanged(sent.reshape(targets, -1, 4, LANES), NEAR).reshape(-1, LANES)
    camera_map, bucket_counts, arrived = lax.optimization_barrier((camera_map, bucket_counts, arrived))
    hot = jnp.argmax(bucket_counts[0])
    ids = camera_map.reshape(4, 2, 4, 2, QUARTERS, SPAN)
    ids = lax.dynamic_slice(ids, (0, 0, 0, core, level, 0), (4, 2, 4, 1, 1, SPAN))
    ids = ids.reshape(4, 8, SPAN).transpose(1, 0, 2).reshape(-1, 2, LANES)
    hot_ids = lax.dynamic_slice_in_dim(camera_map, hot * CAM_DEV + core * 4 * LANES, 4 * LANES)
    hot_ids = jnp.where(level == 0, hot_ids, -1).reshape(-1, 2, LANES)
    ids = jnp.concatenate([ids, hot_ids], axis=0)
    here = jnp.bitwise_and(jnp.right_shift(ids, 10), 31) == lax.axis_index(RANGE)
    codes = jnp.right_shift(ids, 15) * QUARTERS * SPAN + jnp.bitwise_and(ids, QUARTERS * SPAN - 1)
    codes = jnp.where(here & (ids >= 0), codes, -SPAN)
    sums = camera_sums(arrived)
    share = sums[0]
    for turn in range(1, QUARTERS):
        share = share + turned(sums[turn], "zk", turn)
    squares = to_owner(share[GRAD_ROWS:])
    slots = from_all(share[:GRAD_ROWS], RANGE)
    slots, squares = lax.optimization_barrier((slots, squares))
    shares = [squares]
    for turn in range(1, QUARTERS):
        shares.append(turned(squares, "x", turn))
    mine, theirs = placed(slots, codes, 2 * QUARTERS)
    theirs = turned(theirs, "c", 1)
    mine = mine + theirs[: mine.shape[0]]
    part = mine
    for turn in range(1, QUARTERS):
        part = part + turned(mine, "zk", turn)
    blocks = whole_blocks(bucket_counts, shares, slots, theirs)
    spread = jnp.broadcast_to(part[None], (targets // 2, *part.shape))
    part = exchanged(spread, RANGE)
    part, blocks = lax.optimization_barrier((part, blocks))
    other = turned(part, "c", 1)
    core = core.reshape(1)
    gradient = ordered(core, part)
    gradient = ordered(core, other, gradient)
    return gradient, blocks


def solution(mesh):
    split = Mesh(mesh.devices.reshape(4, 2, 4, 2, mesh.shape["rep"]), ALL)
    return jax.shard_map(
        local,
        mesh=split,
        in_specs=(P(None, ALL), P(None, ALL), P(ALL), P(ALL, None), P()),
        out_specs=(P(), P(None, OBS)),
        check_vma=False,
    )
```
